8 devices in a mesh: dp: 1 (over z), tp: 8 (over x, y, core).
Axes of the slice: x: 2, y: 2, z: 1, core: 2. Of those that a mesh axis runs over, the one named last changes fastest.
Arguments:
- x: bfloat16 [4, 512, 8192], P('dp')
- gain_a: bfloat16 [8192], replicated
- wq: bfloat16 [8192, 8192], P(None, 'tp')
- wk: bfloat16 [8192, 1024], P(None, 'tp')
- wv: bfloat16 [8192, 1024], P(None, 'tp')
- wo: bfloat16 [8192, 8192], P('tp')
- gain_m: bfloat16 [8192], replicated
- w_gate: bfloat16 [8192, 28672], P(None, 'tp')
- w_up: bfloat16 [8192, 28672], P(None, 'tp')
- w_down: bfloat16 [28672, 8192], P('tp')
Outputs:
- output: bfloat16 [4, 512, 8192], P('dp')
All inputs are finite; a program needn't handle non-finite values.
Results may differ from the reference program's by a relative error of at most 0.017.
Values are sent between devices in bfloat16 or wider.
A program may use at most 2 GiB of HBM per device.

```python
import jax
import jax.numpy as jnp
from jax import lax

SEQUENCES = 4
TOKENS = 512
D = 8192
HEADS = 64
KV_HEADS = 8
HEAD = 128
FF = 28672
THETA = 10000


def setup_inputs(seed: int = 0, part: int = 0) -> dict:
    kx, ka, km, kq, kk, kv, ko, kg, ku, kd = jax.random.split(jax.random.key(seed), 10)

    def weights(key, rows, columns):
        return jax.random.normal(key, (rows, columns), jnp.float32) * rows**-0.5

    drawn = {
        "x": jax.random.normal(jax.random.fold_in(kx, part), (SEQUENCES, TOKENS, D), jnp.float32),
        "gain_a": 1 + 0.1 * jax.random.normal(ka, (D,), jnp.float32),
        "wq": 2 * weights(kq, D, HEADS * HEAD),
        "wk": 2 * weights(kk, D, KV_HEADS * HEAD),
        "wv": 4 * weights(kv, D, KV_HEADS * HEAD),
        "wo": weights(ko, HEADS * HEAD, D),
        "gain_m": 1 + 0.1 * jax.random.normal(km, (D,), jnp.float32),
        "w_gate": weights(kg, D, FF),
        "w_up": weights(ku, D, FF),
        "w_down": 3 * weights(kd, FF, D),
    }
    return {k: v.astype(jnp.bfloat16) for k, v in drawn.items()}


def normed(x, gain):
    wide = x.astype(jnp.float32)
    scale = lax.rsqrt(jnp.mean(wide * wide, -1, keepdims=True) + 1e-6)
    return (wide * scale * gain.astype(jnp.float32)).astype(jnp.bfloat16)


def turned(t, place, theta):
    half = t.shape[-1] // 2
    angle = place.astype(jnp.float32)[:, None] * theta ** (-jnp.arange(half, dtype=jnp.float32) / half)
    cos, sin = jnp.cos(angle)[:, None], jnp.sin(angle)[:, None]
    a, b = t[..., :half].astype(jnp.float32), t[..., half:].astype(jnp.float32)
    return jnp.concatenate([a * cos - b * sin, b * cos + a * sin], -1).astype(jnp.bfloat16)


def matmul(a, w):
    return jnp.dot(a, w, preferred_element_type=jnp.float32).astype(jnp.bfloat16)


def einsum(form, a, b):
    return jnp.einsum(form, a.astype(jnp.float32), b.astype(jnp.float32))


def attention(q, k, v):
    scores = einsum("tgsd,ugd->gstu", q, k) * q.shape[-1] ** -0.5
    token = jnp.arange(q.shape[0])
    scores = jnp.where(token[:, None] >= token, scores, -jnp.inf)
    weights = jax.nn.softmax(scores, -1).astype(jnp.bfloat16)
    return einsum("gstu,ugd->tgsd", weights, v).astype(jnp.bfloat16)


def one(x, gain_a, wq, wk, wv, wo, gain_m, w_gate, w_up, w_down):
    rows = x.shape[0]
    a, place = normed(x, gain_a), jnp.arange(rows)
    k = turned(matmul(a, wk).reshape(rows, -1, HEAD), place, THETA)
    q = turned(matmul(a, wq).reshape(rows, -1, HEAD), place, THETA).reshape(rows, k.shape[1], -1, HEAD)
    v = matmul(a, wv).reshape(rows, -1, HEAD)
    seen = attention(q, k, v).reshape(rows, -1)
    h = (x.astype(jnp.float32) + jnp.dot(seen, wo, preferred_element_type=jnp.float32)).astype(jnp.bfloat16)
    b = normed(h, gain_m)
    gate = jnp.dot(b, w_gate, preferred_element_type=jnp.float32)
    up = jnp.dot(b, w_up, preferred_element_type=jnp.float32)
    hidden = (jax.nn.silu(gate) * up).astype(jnp.bfloat16)
    return (h.astype(jnp.float32) + jnp.dot(hidden, w_down, preferred_element_type=jnp.float32)).astype(jnp.bfloat16)


def reference(x, gain_a, wq, wk, wv, wo, gain_m, w_gate, w_up, w_down):
    return lax.map(lambda sequence: one(sequence, gain_a, wq, wk, wv, wo, gain_m, w_gate, w_up, w_down), x)
```

```python
import functools

import jax
import jax.numpy as jnp
from jax import lax
from jax.experimental import pallas as pl
from jax.experimental.pallas import tpu as pltpu
from jax.sharding import PartitionSpec as P

HEAD = 128
THETA = 10000
LOG2E = 1.4426950408889634
HIDDEN = -1e30
EPS = 1e-6

CHUNK = 512
SHARD = 64
COLS = 1024
PIECES = 8
BF, F32 = jnp.bfloat16, jnp.float32

LAST = 56
GAP = 10
L_LOAD_A, L_ADD_A, L_LOAD_B, L_ADD_B = 2, 3, 5, 6
L_Y_B, L_Y_A = 8, 10
L_H_B, L_H_A = 15, 17
READY = 21
STEPS = LAST + GAP + PIECES + L_Y_A


def _dot(a, b):
    return jnp.dot(a, b, preferred_element_type=F32)


def _mul(i, n):
    return pl.multiple_of(i * n, n)


def _kernel(cos, sin, gain_a, gain_m, x, wq, wk, wv, wo, wg, wu, wd, y, bbuf, recva, reta, recvb,
            slot, b, hid, xs, q_s, k_s, v_s, vt_s, seen, own, csend, crecv, senda, retas, rt_l, ra_l, sendb, retb, rb_l, res_l, fin, hsh, bsh,
            slot_sem, b_sem, xs_sem, c_send, c_recv, a_send, a_recv, ra_out, la_sem, lt_sem, b_send, b_recv, lb_sem, lr_sem,
            hs_b, hs_a, hs_c, hl, hr_b, hr_a, rc, fw, gs, gl, yr_b, yr_a):
    chunks = x.shape[0] // CHUNK
    h_sums = chunks
    me = lax.axis_index("tp")
    core, iy, ix = lax.rem(me, 2), lax.rem(lax.div(me, 2), 2), lax.div(me, 4)
    d = 1 - 2 * core
    sib, xn, yn = me + d, me + 4 - 8 * ix, me + 2 - 4 * iy
    a_dev, b_dev = xn * (1 - core) + yn * core, yn * (1 - core) + xn * core
    ab = xn + yn - me
    shard_at = [ab + d, b_dev + d, a_dev + d, sib, ab, a_dev, b_dev, me]

    def remote(src, dst, send, recv, to):
        return pltpu.make_async_remote_copy(src_ref=src, dst_ref=dst, send_sem=send, recv_sem=recv, device_id={"tp": to},
                                            device_id_type=pl.DeviceIdType.MESH)

    def start_local(src, dst, sem):
        pltpu.make_async_copy(src, dst, sem).start()

    def wait(ref, sem):
        pltpu.make_async_copy(ref, ref, sem).wait()

    def cols_of(i, n=COLS):
        return pl.ds(_mul(i, n), n)

    def rows_of(c, shard):
        return pl.ds(_mul(c * 8 + shard, SHARD), SHARD)


    def add_core(k):
        u, i, two = lax.div(k, PIECES), lax.rem(k, PIECES), lax.rem(k, 2)
        a_slot = lax.rem(u, 3)

        @pl.when(i >= 1)
        def _():
            wait(retas.at[0], ra_out.at[1 - two])

        @pl.when((i == 0) & (u >= 3))
        def _():
            wait(senda.at[0], a_send.at[a_slot])

        wait(crecv.at[0], c_recv.at[lax.rem(k, 4)])

        @pl.loop(0, 4)
        def _(r):
            up, lo = pl.ds(_mul(r, 32), 32), pl.ds(_mul(r + 4, 32), 32)
            senda[a_slot, up, cols_of(i)] = (own[two, up, :] + crecv[lax.rem(k, 4), up, :].astype(F32)).astype(BF)
            retas[two, up, :] = own[two, lo, :] + crecv[lax.rem(k, 4), lo, :].astype(F32)

        start_local(retas.at[two], reta.at[u, :, cols_of(i)], ra_out.at[two])

    def staged(v, fn):
        ok = (v >= 0) & ((v < LAST) | ((v >= LAST + GAP) & (v < LAST + GAP + PIECES)))

        @pl.when(ok)
        def _():
            k = jnp.where(v < LAST, v, v - GAP)
            fn(k, lax.div(k, PIECES), lax.rem(k, PIECES))

    def send_a(k, u, i):
        part = senda.at[lax.rem(u, 3), :, cols_of(i)]
        remote(part, recva.at[u, :, cols_of(i)], a_send.at[lax.rem(u, 3)], a_recv.at[k], a_dev).start()

    def load_a(k, u, i):
        two = lax.rem(k, 2)
        wait(recva.at[u, :, cols_of(i)], a_recv.at[k])
        start_local(recva.at[u, :, cols_of(i)], ra_l.at[two], la_sem.at[two])
        start_local(reta.at[u, :, cols_of(i)], rt_l.at[two], lt_sem.at[two])

    def add_a(k, u, i):
        two, ring = lax.rem(k, 2), lax.rem(k, 4)
        wait(ra_l.at[two], la_sem.at[two])
        wait(rt_l.at[two], lt_sem.at[two])

        @pl.when(k >= 4)
        def _():
            wait(sendb.at[0], b_send.at[ring])

        @pl.loop(0, 2)
        def _(r):
            up, lo = pl.ds(_mul(r, 32), 32), pl.ds(_mul(r + 2, 32), 32)
            sendb[ring, up, :] = (rt_l[two, up, :] + ra_l[two, up, :].astype(F32)).astype(BF)
            retb[ring, up, :] = rt_l[two, lo, :] + ra_l[two, lo, :].astype(F32)

        remote(sendb.at[ring], recvb.at[u, :, cols_of(i)], b_send.at[ring], b_recv.at[k], b_dev).start()

    def load_b(k, u, i):
        two = lax.rem(k, 2)
        wait(recvb.at[u, :, cols_of(i)], b_recv.at[k])
        start_local(recvb.at[u, :, cols_of(i)], rb_l.at[two], lb_sem.at[two])

        @pl.when(u < h_sums)
        def _():
            start_local(x.at[rows_of(u, me), cols_of(i)], res_l.at[two], lr_sem.at[two])

    def add_b(k, u, i):
        two, four, ring = lax.rem(k, 2), lax.rem(k, 4), lax.rem(k, 8)
        wait(rb_l.at[two], lb_sem.at[two])

        @pl.when(u < h_sums)
        def _():
            wait(res_l.at[two], lr_sem.at[two])

            @pl.loop(0, 2)
            def _(r):
                at = pl.ds(_mul(r, 32), 32)
                total = retb[four, at, :] + rb_l[two, at, :].astype(F32)
                hsh[u, at, cols_of(i)] = (res_l[two, at, :].astype(F32) + total).astype(BF)

            @pl.when(i == PIECES - 1)
            def _():
                norm_h(u)

        @pl.when(u >= h_sums)
        def _():
            c = u - h_sums

            @pl.when(k >= h_sums * PIECES + 8)
            def _():
                wait(csend.at[0, pl.ds(0, 3 * SHARD)], gs.at[ring])
                wait(fin.at[0], gl.at[ring])

            @pl.loop(0, 2)
            def _(r):
                at = pl.ds(_mul(r, 32), 32)
                total = retb[four, at, :] + rb_l[two, at, :].astype(F32)
                fin[ring, at, :] = (hsh[c, at, cols_of(i)].astype(F32) + total).astype(BF)

            mine, n = y.at[rows_of(c, me), cols_of(i)], k - h_sums * PIECES
            remote(fin.at[ring], mine, gs.at[ring], yr_b.at[n], b_dev).start()
            remote(fin.at[ring], mine, gs.at[ring], yr_a.at[n], a_dev).start()
            remote(fin.at[ring], mine, gs.at[ring], rc.at[u], sib).start()
            start_local(fin.at[ring], mine, gl.at[ring])

    def norm_rows(src, dst, gain, groups):
        @pl.loop(0, groups)
        def _(r):
            squares = jnp.zeros((16, 1024), F32)
            for j in range(8):
                wide = src(r, j).astype(F32)
                squares += wide * wide
            scale = lax.rsqrt(jnp.sum(squares, -1, keepdims=True) * (1 / 8192) + EPS)
            for j in range(8):
                dst(r, j, (src(r, j).astype(F32) * scale * gain[:, j * 1024 : (j + 1) * 1024]).astype(BF))

    def norm_h(u):
        @pl.when(u >= 1)
        def _():
            for sem in (hs_b, hs_a, hs_c):
                wait(bsh, sem)

        def src(r, j):
            return hsh[u, pl.ds(_mul(r, 16), 16), j * 1024 : (j + 1) * 1024]

        def dst(r, j, value):
            bsh[pl.ds(_mul(r, 16), 16), j * 1024 : (j + 1) * 1024] = value

        norm_rows(src, dst, gain_m, 4)
        start_local(bsh, bbuf.at[rows_of(u, me)], hl)

        @pl.loop(0, 4)
        def _(q):
            part, mine = bsh.at[:, cols_of(q, 2048)], bbuf.at[rows_of(u, me), cols_of(q, 2048)]
            remote(part, mine, hs_b, hr_b.at[u * 4 + q], b_dev).start()
            remote(part, mine, hs_a, hr_a.at[u * 4 + q], a_dev).start()
            remote(part, mine, hs_c, rc.at[u], sib).start()

    def staged_h(v, fn):
        ok = (v >= 0) & (v < h_sums * PIECES) & (lax.rem(v, PIECES) < 4)

        @pl.when(ok)
        def _():
            fn(lax.div(v, PIECES), lax.rem(v, PIECES))

    def pass_h_b(u, q):
        @pl.when(q == 0)
        def _():
            wait(bsh, hl)

        part = bbuf.at[rows_of(u, b_dev), cols_of(q, 2048)]
        wait(part, hr_b.at[u * 4 + q])
        remote(part, part, fw.at[u], hr_a.at[u * 4 + q], a_dev).start()
        remote(part, part, fw.at[u], rc.at[u], sib).start()

    def pass_h_a(u, q):
        wait(recva.at[u, :, cols_of(q, 2048)], hr_a.at[u * 4 + q])
        for who in (a_dev, ab):
            part = bbuf.at[rows_of(u, who), cols_of(q, 2048)]
            remote(part, part, fw.at[u], rc.at[u], sib).start()

    def pass_y_b(k, u, i):
        @pl.when(u >= h_sums)
        def _():
            part, n = y.at[rows_of(u - h_sums, b_dev), cols_of(i)], k - h_sums * PIECES
            wait(part, yr_b.at[n])
            remote(part, part, fw.at[u], yr_a.at[n], a_dev).start()
            remote(part, part, fw.at[u], rc.at[u], sib).start()

    def pass_y_a(k, u, i):
        @pl.when(u >= h_sums)
        def _():
            wait(recva.at[u, :, cols_of(i)], yr_a.at[k - h_sums * PIECES])
            for who in (a_dev, ab):
                part = y.at[rows_of(u - h_sums, who), cols_of(i)]
                remote(part, part, fw.at[u], rc.at[u], sib).start()

    def exchange(first, end):
        @pl.loop(first, end)
        def _(v):
            staged(v, send_a)
            staged(v - L_LOAD_A, load_a)
            staged(v - L_ADD_A, add_a)
            staged(v - L_LOAD_B, load_b)
            staged(v - L_ADD_B, add_b)
            staged_h(v - L_H_B, pass_h_b)
            staged(v - L_Y_B, pass_y_b)
            staged_h(v - L_H_A, pass_h_a)
            staged(v - L_Y_A, pass_y_a)


    def load_q(half, s):
        start_local(wq.at[:, cols_of(half, 512)], slot.at[s], slot_sem.at[s])

    def load_kv(s):
        start_local(wk, slot.at[s, :, pl.ds(0, HEAD)], slot_sem.at[s])
        start_local(wv, slot.at[s, :, pl.ds(HEAD, HEAD)], slot_sem.at[s])

    def load_wo(half, s):
        for n in range(8):
            start_local(wo.at[:, cols_of(half * 8 + n, 512)], slot.at[s, pl.ds(n * 1024, 1024)], slot_sem.at[s])

    def load_gu(t, s):
        start_local(wg.at[:, cols_of(t, 256)], slot.at[s, :, pl.ds(0, 256)], slot_sem.at[s])
        start_local(wu.at[:, cols_of(t, 256)], slot.at[s, :, pl.ds(256, 256)], slot_sem.at[s])

    def load_d(t, s):
        for n in range(2):
            start_local(wd.at[:, cols_of(t * 2 + n, 512)], slot.at[s, pl.ds(n * 3584, 3584)], slot_sem.at[s])


    def produce(k, tile):
        ring, two = lax.rem(k, 4), lax.rem(k, 2)

        @pl.when(k >= 2)
        def _():
            wait(csend.at[0], c_send.at[two])

        for n in range(2):
            term = tile(n)
            csend[two, :, n * 512 : (n + 1) * 512] = term[:256].astype(BF)
            own[two, :, n * 512 : (n + 1) * 512] = term[256:]
        remote(csend.at[two], crecv.at[ring], c_send.at[two], c_recv.at[ring], sib).start()

    def finish(u):
        add_core(u * PIECES + PIECES - 1)
        wait(retas.at[0], ra_out.at[1])

    def turn(t):
        wide = t.astype(BF).astype(F32)
        return (wide * cos[...] + pltpu.roll(wide, HEAD // 2, 1) * sin[...]).astype(BF)

    def norm_x(c):
        def load(i, s):
            start_local(x.at[pl.ds(_mul(c * 16 + i, 32), 32)], xs.at[s], xs_sem.at[s])

        load(0, 0)

        @pl.loop(0, 16)
        def _(i):
            s = lax.rem(i, 2)

            @pl.when(i < 15)
            def _():
                load(i + 1, 1 - s)

            wait(xs.at[s], xs_sem.at[s])

            def src(r, j):
                return xs[s, pl.ds(_mul(r, 16), 16), j * 1024 : (j + 1) * 1024]

            def dst(r, j, value):
                b[pl.ds(_mul(i * 2 + r, 16), 16), j * 1024 : (j + 1) * 1024] = value

            norm_rows(src, dst, gain_a, 2)

    def attention():
        vt_s[0:HEAD, :] = v_s[...].T
        key = lax.broadcasted_iota(jnp.int32, (256, 256), 0)
        query = lax.broadcasted_iota(jnp.int32, (256, 256), 1)
        ok = key <= query
        e = HEAD**-0.5 * LOG2E

        def place(i):
            iy_, ix_, core_ = (i // 2) % 2, i // 4, i % 2
            fx, fy, fc = (ix_ - ix) * (ix_ - ix), (iy_ - iy) * (iy_ - iy), (core_ - core) * (core_ - core)
            fa, fb = fx * (1 - core) + fy * core, fy * (1 - core) + fx * core
            return (1 - fc) * (7 - 2 * fa - fb) + fc * (3 - fa - 2 * fb)

        @pl.loop(0, 8)
        def _(h):
            def scores(kb, qb):
                return lax.dot_general(k_s[kb * 256 : (kb + 1) * 256, :], q_s[h, qb * 256 : (qb + 1) * 256, :],
                                       (((1,), (1,)), ((), ())), preferred_element_type=F32)

            def put(qb, total):
                out = (total[:HEAD] * (1 / total[HEAD : HEAD + 1])).T.astype(BF)
                for j in range(4):
                    seen[pl.ds(_mul(place(qb * 4 + j), SHARD), SHARD), pl.ds(_mul(h, HEAD), HEAD)] = out[j * SHARD : (j + 1) * SHARD]

            s00 = jnp.where(ok, scores(0, 0), HIDDEN)
            s01 = scores(0, 1)
            s11 = jnp.where(ok, scores(1, 1), HIDDEN)
            top0 = jnp.max(s00, axis=0, keepdims=True)
            top1 = jnp.maximum(jnp.max(s01, axis=0, keepdims=True), jnp.max(s11, axis=0, keepdims=True))
            p00 = jnp.exp2((s00 - top0) * e).astype(BF)
            p01 = jnp.exp2((s01 - top1) * e).astype(BF)
            p11 = jnp.exp2((s11 - top1) * e).astype(BF)
            put(0, _dot(vt_s[:, 0:256], p00))
            put(1, _dot(vt_s[:, 0:256], p01) + _dot(vt_s[:, 256:512], p11))


    barrier = pltpu.get_barrier_semaphore()
    for other in (sib, a_dev, b_dev):
        pl.semaphore_signal(barrier, inc=1, device_id={"tp": other}, device_id_type=pl.DeviceIdType.MESH)
    load_q(0, 0)
    vt_s[HEAD:, :] = jnp.ones((16, CHUNK), BF)
    pl.semaphore_wait(barrier, 3)

    def a_steps(tau):
        return jnp.where(tau < 3, 0, jnp.where(tau == 3, 3, tau + 1))

    @pl.loop(0, chunks)
    def _(c):
        norm_x(c)

        def service(s):
            tau = 5 * c + s
            exchange(a_steps(tau - 1), a_steps(tau))

        @pl.loop(0, 2)
        def _(half):
            s = lax.rem(5 * c + half, 2)

            @pl.when(half == 0)
            def _():
                load_q(1, 1 - s)

            @pl.when(half == 1)
            def _():
                load_kv(1 - s)

            wait(slot.at[s], slot_sem.at[s])
            for n in range(2):
                r = _dot(b[...], slot[s, :, n * 256 : (n + 1) * 256])
                for m in range(2):
                    q_s[half * 4 + n * 2 + m] = turn(r[:, m * HEAD : (m + 1) * HEAD])
            service(half)

        s = lax.rem(5 * c + 2, 2)
        load_wo(0, 1 - s)
        wait(slot.at[s, :, pl.ds(0, 256)], slot_sem.at[s])
        r = _dot(b[...], slot[s, :, 0:256])
        k_s[...] = turn(r[:, :HEAD])
        v_s[...] = r[:, HEAD:].astype(BF)
        attention()
        service(2)

        @pl.loop(0, 2)
        def _(half):
            s = lax.rem(5 * c + 3 + half, 2)

            @pl.when(half == 0)
            def _():
                load_wo(1, 1 - s)

            @pl.when((half == 1) & (c < chunks - 1))
            def _():
                load_q(0, 1 - s)

            @pl.when((half == 1) & (c == chunks - 1))
            def _():
                load_gu(0, 1 - s)

            wait(slot.at[s], slot_sem.at[s])

            @pl.loop(0, 4)
            def _(p):
                i = half * 4 + p
                k = c * PIECES + i
                produce(k, lambda n: _dot(seen[...], slot[s, pl.ds(_mul(p * 2 + n, 1024), 1024), :]))

                @pl.when(i >= 1)
                def _():
                    add_core(k - 1)

            @pl.when(half == 1)
            def _():
                finish(c)

            service(3 + half)

    exchange(a_steps(5 * chunks - 1), READY)

    def fetch_b(c):
        wait(recva.at[pl.ds(0, 2)], rc.at[c])
        for p in range(8):
            start_local(bbuf.at[rows_of(c, shard_at[p])], b.at[pl.ds(p * SHARD, SHARD)], b_sem)

    def m_steps(sigma):
        s = sigma + 1
        first = READY + lax.div(s * 8, 14)
        second = 29 + lax.div((s - 14) * 9, 22)
        third = 38 + lax.div((s - 36) * 10, 22)
        fourth = 48 + lax.div((s - 58) * 18, 22)
        last = LAST + GAP + s - 81
        return jnp.where(s <= 14, first, jnp.where(s <= 36, second, jnp.where(s <= 58, third, jnp.where(s <= 80, fourth, last))))

    fetch_b(0)

    @pl.loop(0, chunks)
    def _(c):
        u = h_sums + c
        wait(b, b_sem)

        def service(t):
            sigma = 22 * c + t
            exchange(m_steps(sigma - 1), m_steps(sigma))

        @pl.loop(0, 14)
        def _(t):
            s = lax.rem(t, 2)

            @pl.when(t < 13)
            def _():
                load_gu(t + 1, 1 - s)

            @pl.when(t == 13)
            def _():
                load_d(0, 1 - s)

            wait(slot.at[s], slot_sem.at[s])
            gate = _dot(b[...], slot[s, :, 0:256])
            up = _dot(b[...], slot[s, :, 256:512])
            hid[:, cols_of(t, 256)] = (gate * jax.nn.sigmoid(gate) * up).astype(BF)
            service(t)

        @pl.when(c < chunks - 1)
        def _():
            fetch_b(c + 1)

        @pl.loop(0, 8)
        def _(t):
            s = lax.rem(t, 2)

            @pl.when(t < 7)
            def _():
                load_d(t + 1, 1 - s)

            @pl.when((t == 7) & (c < chunks - 1))
            def _():
                load_gu(0, 1 - s)

            wait(slot.at[s, pl.ds(0, 7168)], slot_sem.at[s])
            k = u * PIECES + t
            produce(k, lambda n: _dot(hid[...], slot[s, pl.ds(n * 3584, 3584), :]))

            @pl.when(t >= 1)
            def _():
                add_core(k - 1)

            @pl.when(t == 7)
            def _():
                finish(u)

            service(14 + t)

    exchange(m_steps(22 * chunks - 1), STEPS)

    sums = 2 * chunks
    for n in range(4):
        wait(sendb.at[0], b_send.at[n])
    for n in range(2):
        wait(csend.at[0], c_send.at[n])
    for n in range(3):
        wait(senda.at[0], a_send.at[n])
    for n in range(8):
        wait(csend.at[0, pl.ds(0, 3 * SHARD)], gs.at[n])
        wait(fin.at[0], gl.at[n])
    for sem in (hs_b, hs_a, hs_c):
        wait(bsh, sem)
    for n in range(sums):
        wait(recva.at[pl.ds(0, 2)], fw.at[n])
    for n in range(chunks, sums):
        wait(recva.at[pl.ds(0, 2)], rc.at[n])


def _layer(x, gain_a, wq, wk, wv, wo, gain_m, wg, wu, wd):
    tokens, width = x.shape
    chunks = tokens // CHUNK
    sums, pieces = 2 * chunks, 2 * chunks * PIECES
    half = HEAD // 2
    angle = jnp.arange(CHUNK, dtype=F32)[:, None] * THETA ** (-jnp.arange(half, dtype=F32) / half)
    cos, sin = jnp.cos(angle), jnp.sin(angle)
    cos, sin = jnp.concatenate([cos, cos], 1), jnp.concatenate([-sin, sin], 1)
    gains = [g.astype(F32).reshape(1, width) for g in (gain_a, gain_m)]
    any_, vmem = pl.BlockSpec(memory_space=pl.ANY), pl.BlockSpec(memory_space=pltpu.VMEM)
    dma = pltpu.SemaphoreType.DMA
    ff = wg.shape[1]
    matmuls = tokens * (wq.shape[1] * 2 + 2 * HEAD + 3 * ff)
    out = pl.pallas_call(
        _kernel,
        out_shape=[
            jax.ShapeDtypeStruct((tokens, width), BF),
            jax.ShapeDtypeStruct((tokens, width), BF),
            jax.ShapeDtypeStruct((sums, 2 * SHARD, width), BF),
            jax.ShapeDtypeStruct((sums, 2 * SHARD, width), F32),
            jax.ShapeDtypeStruct((sums, SHARD, width), BF),
        ],
        in_specs=[vmem] * 4 + [any_] * 8,
        out_specs=[any_] * 5,
        scratch_shapes=[
            pltpu.VMEM((2, 8192, 512), BF),
            pltpu.VMEM((CHUNK, width), BF),
            pltpu.VMEM((CHUNK, ff), BF),
            pltpu.VMEM((2, SHARD // 2, width), BF),
            pltpu.VMEM((8, CHUNK, HEAD), BF),
            pltpu.VMEM((CHUNK, HEAD), BF),
            pltpu.VMEM((CHUNK, HEAD), BF),
            pltpu.VMEM((HEAD + 16, CHUNK), BF),
            pltpu.VMEM((CHUNK, 8 * HEAD), BF),
            pltpu.VMEM((2, 256, COLS), F32),
            pltpu.VMEM((2, 256, COLS), BF),
            pltpu.VMEM((4, 256, COLS), BF),
            pltpu.VMEM((3, 128, width), BF),
            pltpu.VMEM((2, 128, COLS), F32),
            pltpu.VMEM((2, 128, COLS), F32),
            pltpu.VMEM((2, 128, COLS), BF),
            pltpu.VMEM((4, SHARD, COLS), BF),
            pltpu.VMEM((4, SHARD, COLS), F32),
            pltpu.VMEM((2, SHARD, COLS), BF),
            pltpu.VMEM((2, SHARD, COLS), BF),
            pltpu.VMEM((8, SHARD, COLS), BF),
            pltpu.VMEM((chunks, SHARD, width), BF),
            pltpu.VMEM((SHARD, width), BF),
            dma((2,)), dma, dma((2,)),
            dma((2,)), dma((4,)),
            dma((3,)), dma((pieces,)), dma((2,)), dma((2,)), dma((2,)),
            dma((4,)), dma((pieces,)), dma((2,)), dma((2,)),
            dma, dma, dma, dma,
            dma((chunks * 4,)), dma((chunks * 4,)), dma((sums,)), dma((sums,)),
            dma((8,)), dma((8,)), dma((pieces // 2,)), dma((pieces // 2,)),
        ],
        compiler_params=pltpu.CompilerParams(collective_id=0, has_side_effects=True, vmem_limit_bytes=67043328),
        cost_estimate=pl.CostEstimate(flops=2 * width * matmuls, transcendentals=0, bytes_accessed=10**9),
    )(cos, sin, *gains, x, wq, wk, wv, wo, wg, wu, wd)
    return out[0]


def solution(mesh):
    def step(x, *rest):
        return _layer(x.reshape(-1, x.shape[-1]), *rest).reshape(x.shape)

    tokens, whole, columns, rows = P("dp", None, None), P(None), P(None, "tp"), P("tp", None)
    return jax.shard_map(
        step,
        mesh=mesh,
        in_specs=(tokens, whole, columns, columns, columns, rows, whole, columns, columns, rows),
        out_specs=tokens,
        check_vma=False,
    )
```

```python
import jax
import jax.numpy as jnp
import numpy as np
from jax import lax
from jax.experimental import pallas as pl
from jax.experimental.pallas import tpu as pltpu
from jax.sharding import PartitionSpec as P

HEAD = 128
THETA = 10000
LOG2E = 1.4426950408889634
HIDDEN = -1e30
EPS = 1e-6

CHUNK = 512
SHARD = 64
COLS = 1024
PIECES = 8
BF, F32 = jnp.bfloat16, jnp.float32

STRIDE, LAG = 16, 4
L_LOAD_A, L_ADD_A = LAG, LAG + 2
L_LOAD_B, L_ADD_B = 2 * LAG + 2, 2 * LAG + 4
L_Y_B, L_Y_A = 3 * LAG + 4, 4 * LAG + 4
L_H, L_H_B, L_H_A = 2 * LAG + 12, 3 * LAG + 12, 4 * LAG + 12
WAIT = 4
PACE = (
    "00001111101211102202212120000100010110100105",
    "2201101011112222110101",
    "0111122221101011011101",
    "2110111011110222021011",
    "0111101222120001111112",
)


def _counts():
    return [int(digit) for digit in "".join(PACE)]


def _packed():
    counts = _counts()
    totals = [sum(counts[: n + 1]) for n in range(len(counts))]
    return [totals[n] + sum((totals[n + m] - totals[n]) << (3 + 5 * m) for m in (1, 2, 3)) for n in range(0, len(totals), 4)]


def _done(g):
    words = _packed()
    word = jnp.int32(words[-1])
    for n in reversed(range(len(words) - 1)):
        word = jnp.where(g < 4 * n + 4, words[n], word)
    m = g & 3
    total = (word & 255) + jnp.where(m == 0, 0, lax.shift_right_logical(word, 3 + 5 * m) & 31)
    return jnp.where(g < 0, 0, total)


def _dot(a, b):
    return jnp.dot(a, b, preferred_element_type=F32)


def _at(i, n):
    return slice(i * n, i * n + n)


def _mul(i, n):
    return pl.multiple_of(i * n, n)


def _kernel(turns, gains, x, wq, wk, wv, wo, wg, wu, wd, y, bbuf, recva, reta, recvb,
            slot, b, hid, gain_s, vt_s, seen, own, csend, crecv, senda, retas, rt_l, ra_l, sendb, retb, rb_l, res_l, hsh, shard,
            slot_sem, b_sem, xs_sem, c_send, c_recv, a_send, a_recv, ra_out, la_sem, lt_sem, b_send, b_recv, lb_sem, lr_sem,
            sh_b, sh_a, sh_c, sh_l, from_b, from_a, rc, fw):
    chunks = x.shape[0] // CHUNK
    h_sums, sums = chunks, 2 * chunks
    me = lax.axis_index("tp")
    core, iy, ix = lax.rem(me, 2), lax.rem(lax.div(me, 2), 2), lax.div(me, 4)
    d = 1 - 2 * core
    sib, xn, yn = me + d, me + 4 - 8 * ix, me + 2 - 4 * iy
    a_dev, b_dev = xn * (1 - core) + yn * core, yn * (1 - core) + xn * core
    ab = xn + yn - me

    keys = pl.ds(8 * HEAD, HEAD)

    def remote(src, dst, send, recv, to):
        return pltpu.make_async_remote_copy(src_ref=src, dst_ref=dst, send_sem=send, recv_sem=recv, device_id={"tp": to},
                                            device_id_type=pl.DeviceIdType.MESH)

    def start_local(src, dst, sem):
        pltpu.make_async_copy(src, dst, sem).start()

    def wait(ref, sem):
        pltpu.make_async_copy(ref, ref, sem).wait()

    def cols_of(i, n=COLS):
        return pl.ds(_mul(i, n), n)

    def sixteen(r):
        return pl.ds(_mul(r, 16), 16)

    def thirty_two(r):
        return pl.ds(_mul(r, 32), 32)

    def rows_of(c, shard):
        return pl.ds(_mul(c * 8 + shard, SHARD), SHARD)


    def add_core(k):
        u, i, two = lax.div(k, PIECES), lax.rem(k, PIECES), lax.rem(k, 2)
        a_slot = lax.rem(u, 3)

        @pl.when(i >= 1)
        def _():
            wait(retas.at[0], ra_out.at[1 - two])

        @pl.when((i == 0) & (u >= 3))
        def _():
            wait(senda.at[0], a_send.at[a_slot])

        wait(crecv.at[0], c_recv.at[lax.rem(k, 4)])

        @pl.loop(0, 4)
        def _(r):
            up, lo = thirty_two(r), thirty_two(r + 4)
            senda[a_slot, up, cols_of(i)] = (own[two, up, :] + crecv[lax.rem(k, 4), up, :].astype(F32)).astype(BF)
            retas[two, up, :] = own[two, lo, :] + crecv[lax.rem(k, 4), lo, :].astype(F32)

        start_local(retas.at[two], reta.at[u, :, cols_of(i)], ra_out.at[two])

    def staged(v, fn, first, end):
        if end == sums:
            v = jnp.where(v >= STRIDE * (sums - 1) - WAIT, v - WAIT, v)
        i = v & (STRIDE - 1)

        @pl.when((v >= STRIDE * first) & (v < STRIDE * end) & (i < PIECES))
        def _():
            u = lax.div(v, STRIDE)
            fn(u * PIECES + i, u, i)

    def send_a(k, u, i):
        part = senda.at[lax.rem(u, 3), :, cols_of(i)]
        remote(part, recva.at[u, :, cols_of(i)], a_send.at[lax.rem(u, 3)], a_recv.at[k], a_dev).start()

    def load_a(k, u, i):
        four = k & 3
        wait(recva.at[u, :, cols_of(i)], a_recv.at[k])
        start_local(recva.at[u, :, cols_of(i)], ra_l.at[four], la_sem.at[four])
        start_local(reta.at[u, :, cols_of(i)], rt_l.at[four], lt_sem.at[four])

    def add_a(k, u, i):
        four, ring = k & 3, k & 7
        wait(ra_l.at[four], la_sem.at[four])
        wait(rt_l.at[four], lt_sem.at[four])

        @pl.when(k >= 4)
        def _():
            wait(sendb.at[0], b_send.at[four])

        @pl.loop(0, 2)
        def _(r):
            up, lo = thirty_two(r), thirty_two(r + 2)
            sendb[four, up, :] = (rt_l[four, up, :] + ra_l[four, up, :].astype(F32)).astype(BF)
            retb[ring, up, :] = rt_l[four, lo, :] + ra_l[four, lo, :].astype(F32)

        remote(sendb.at[four], recvb.at[u, :, cols_of(i)], b_send.at[four], b_recv.at[k], b_dev).start()

    def load_b(k, u, i):
        four = k & 3
        wait(recvb.at[u, :, cols_of(i)], b_recv.at[k])
        start_local(recvb.at[u, :, cols_of(i)], rb_l.at[four], lb_sem.at[four])

        @pl.when(u < h_sums)
        def _():
            start_local(x.at[rows_of(u, me), cols_of(i)], res_l.at[four], lr_sem.at[four])

    def add_b(k, u, i):
        four, ring, slot_u = k & 3, k & 7, u & 1
        wait(rb_l.at[four], lb_sem.at[four])

        @pl.when((i == 0) & (u >= 2))
        def _():
            for sem in (sh_b, sh_a, sh_c):
                wait(shard.at[0], sem.at[slot_u])

        @pl.when((i == 0) & (u >= h_sums + 2))
        def _():
            wait(shard.at[0], sh_l.at[slot_u])

        @pl.when(u < h_sums)
        def _():
            wait(res_l.at[four], lr_sem.at[four])

            @pl.loop(0, 2)
            def _(r):
                at = thirty_two(r)
                total = retb[ring, at, :] + rb_l[four, at, :].astype(F32)
                hsh[u, at, cols_of(i)] = (res_l[four, at, :].astype(F32) + total).astype(BF)

            @pl.when(i == PIECES - 1)
            def _():
                norm_h(u, slot_u)

        @pl.when(u >= h_sums)
        def _():
            c = u - h_sums

            @pl.loop(0, 2)
            def _(r):
                at = thirty_two(r)
                total = retb[ring, at, :] + rb_l[four, at, :].astype(F32)
                shard[slot_u, at, cols_of(i)] = (hsh[c, at, cols_of(i)].astype(F32) + total).astype(BF)

            send_shard(y, c, k, u, i)

            @pl.when(i == PIECES - 1)
            def _():
                start_local(shard.at[slot_u], y.at[rows_of(c, me)], sh_l.at[slot_u])

    def halves(i):
        return pl.ds(_mul(lax.div(i, 4), 4096), 4096)

    def send_shard(out, c, k, u, i):
        slot_u = lax.rem(u, 2)
        part, mine = shard.at[slot_u, :, cols_of(i)], out.at[rows_of(c, me), cols_of(i)]
        remote(part, mine, sh_b.at[slot_u], from_b.at[k], b_dev).start()
        remote(part, mine, sh_a.at[slot_u], from_a.at[lax.div(k, 4)], a_dev).start()

        @pl.when((i & 3) == 3)
        def _():
            remote(shard.at[slot_u, :, halves(i)], out.at[rows_of(c, me), halves(i)], sh_c.at[slot_u], rc.at[u], sib).start()

    def pass_b(out, c, k, u, i):
        part = out.at[rows_of(c, b_dev), cols_of(i)]
        wait(part, from_b.at[k])
        remote(part, part, fw.at[u], from_a.at[lax.div(k, 4)], a_dev).start()

        @pl.when((i & 3) == 3)
        def _():
            half = out.at[rows_of(c, b_dev), halves(i)]
            remote(half, half, fw.at[u], rc.at[u], sib).start()

    def pass_a(out, c, k, u, i):
        @pl.when((i & 3) == 3)
        def _():
            wait(recva.at[u, :, halves(i)], from_a.at[lax.div(k, 4)])
            for who in (a_dev, ab):
                half = out.at[rows_of(c, who), halves(i)]
                remote(half, half, fw.at[u], rc.at[u], sib).start()

    def norm_rows(src, dst, which, r):
        squares = jnp.zeros((16, 1024), F32)
        for j in range(8):
            wide = src(r, j).astype(F32)
            squares += wide * wide
        scale = lax.rsqrt(jnp.sum(squares, -1, keepdims=True) * (1 / 8192) + EPS)
        for j in range(8):
            dst(r, j, (src(r, j).astype(F32) * scale * gain_s[which : which + 1, _at(j, COLS)]).astype(BF))

    def norm_h(u, slot_u):
        def src(r, j):
            return hsh[u, sixteen(r), _at(j, COLS)]

        def dst(r, j, value):
            shard[slot_u, sixteen(r), _at(j, COLS)] = value

        @pl.loop(0, 4)
        def _(r):
            norm_rows(src, dst, 1, r)

        start_local(shard.at[slot_u], bbuf.at[rows_of(u, me)], sh_l.at[slot_u])

    def send_h(k, u, i):
        send_shard(bbuf, u, k, u, i)

    def pass_h_b(k, u, i):
        @pl.when(i == 0)
        def _():
            wait(shard.at[0], sh_l.at[lax.rem(u, 2)])

        pass_b(bbuf, u, k, u, i)

    def pass_h_a(k, u, i):
        pass_a(bbuf, u, k, u, i)

    def pass_y_b(k, u, i):
        pass_b(y, u - h_sums, k, u, i)

    def pass_y_a(k, u, i):
        pass_a(y, u - h_sums, k, u, i)

    def exchange(first, end):
        @pl.loop(first, end)
        def _(v):
            staged(v, send_a, 0, sums)
            staged(v - L_LOAD_A, load_a, 0, sums)
            staged(v - L_ADD_A, add_a, 0, sums)
            staged(v - L_LOAD_B, load_b, 0, sums)
            staged(v - L_ADD_B, add_b, 0, sums)

            @pl.when((v >= L_H) & (v < STRIDE * (h_sums - 1) + PIECES + L_H_A))
            def _():
                staged(v - L_H, send_h, 0, h_sums)
                staged(v - L_H_B, pass_h_b, 0, h_sums)
                staged(v - L_H_A, pass_h_a, 0, h_sums)

            @pl.when(v >= STRIDE * h_sums + L_Y_B)
            def _():
                staged(v - L_Y_B, pass_y_b, h_sums, sums)
                staged(v - L_Y_A, pass_y_a, h_sums, sums)


    def load_q(half, s):
        start_local(wq.at[:, cols_of(half, 512)], slot.at[s], slot_sem.at[s])

    def load_kv(s):
        start_local(wk, slot.at[s, :, pl.ds(0, HEAD)], slot_sem.at[s])
        start_local(wv, slot.at[s, :, pl.ds(HEAD, HEAD)], slot_sem.at[s])

    def load_wo(half, s):
        for n in range(8):
            start_local(wo.at[:, cols_of(half * 8 + n, 512)], slot.at[s, pl.ds(n * 1024, 1024)], slot_sem.at[s])

    def load_gu(t, s):
        start_local(wg.at[:, cols_of(t, 256)], slot.at[s, :, pl.ds(0, 256)], slot_sem.at[s])
        start_local(wu.at[:, cols_of(t, 256)], slot.at[s, :, pl.ds(256, 256)], slot_sem.at[s])

    def load_d(t, s):
        for n in range(2):
            start_local(wd.at[:, cols_of(t * 2 + n, 512)], slot.at[s, pl.ds(n * 3584, 3584)], slot_sem.at[s])


    def produce(k, tile, beside=None):
        ring, two = lax.rem(k, 4), lax.rem(k, 2)

        @pl.when(k >= 2)
        def _():
            wait(csend.at[0], c_send.at[two])

        for n in range(2):
            term = tile(n)
            csend[two, :, _at(n, 512)] = term[:256].astype(BF)
            own[two, :, _at(n, 512)] = term[256:]
            if beside and n == 0:
                beside()
        remote(csend.at[two], crecv.at[ring], c_send.at[two], c_recv.at[ring], sib).start()

    def finish(u):
        add_core(u * PIECES + PIECES - 1)

    def flush():
        wait(retas.at[0], ra_out.at[1])

    def turn(t):
        wide = t.astype(BF).astype(F32)
        return (wide * turns[:, :HEAD] + pltpu.roll(wide, HEAD // 2, 1) * turns[:, HEAD:]).astype(BF)

    def load_x(c):
        for i in range(8):
            start_local(x.at[rows_of(c, i)], b.at[pl.ds(i * SHARD, SHARD)], xs_sem.at[i])

    def norm_x(i):
        def src(r, j):
            return b[sixteen(i * 4 + r), _at(j, COLS)]

        def dst(r, j, value):
            b[sixteen(i * 4 + r), _at(j, COLS)] = value

        for r in range(4):
            norm_rows(src, dst, 0, r)

    def attention():
        key = lax.broadcasted_iota(jnp.int32, (256, 256), 0)
        query = lax.broadcasted_iota(jnp.int32, (256, 256), 1)
        ok = key <= query
        e = HEAD**-0.5 * LOG2E

        def place(i):
            iy_, ix_, core_ = (i // 2) % 2, i // 4, i % 2
            fx, fy, fc = (ix_ - ix) * (ix_ - ix), (iy_ - iy) * (iy_ - iy), (core_ - core) * (core_ - core)
            fa, fb = fx * (1 - core) + fy * core, fy * (1 - core) + fx * core
            return (1 - fc) * (7 - 2 * fa - fb) + fc * (3 - fa - 2 * fb)

        def head(h):
            def scores(kb, qb):
                return lax.dot_general(hid[_at(kb, 256), keys], hid[_at(qb, 256), pl.ds(_mul(h, HEAD), HEAD)],
                                       (((1,), (1,)), ((), ())), preferred_element_type=F32)

            def put(qb, total):
                out = (total[:HEAD] * (1 / total[HEAD : HEAD + 1])).T.astype(BF)
                for j in range(4):
                    seen[pl.ds(_mul(place(qb * 4 + j), SHARD), SHARD), pl.ds(_mul(h, HEAD), HEAD)] = out[_at(j, SHARD)]

            s00 = jnp.where(ok, scores(0, 0), HIDDEN)
            s01 = scores(0, 1)
            s11 = jnp.where(ok, scores(1, 1), HIDDEN)
            top0 = jnp.max(s00, axis=0, keepdims=True)
            top1 = jnp.maximum(jnp.max(s01, axis=0, keepdims=True), jnp.max(s11, axis=0, keepdims=True))
            p00 = jnp.exp2((s00 - top0) * e).astype(BF)
            p01 = jnp.exp2((s01 - top1) * e).astype(BF)
            p11 = jnp.exp2((s11 - top1) * e).astype(BF)
            put(0, _dot(vt_s[:, 0:256], p00))
            put(1, _dot(vt_s[:, 0:256], p01) + _dot(vt_s[:, 256:512], p11))

        @pl.loop(0, 4)
        def _(h):
            head(2 * h)
            head(2 * h + 1)


    barrier = pltpu.get_barrier_semaphore()
    for other in (sib, a_dev, b_dev):
        pl.semaphore_signal(barrier, inc=1, device_id={"tp": other}, device_id_type=pl.DeviceIdType.MESH)
    load_x(0)
    load_q(0, 0)
    for n in range(2):
        for j in range(64):
            gain_s[n : n + 1, _at(j, 128)] = gains[n * 64 + j : n * 64 + j + 1, :]
    vt_s[HEAD:, :] = jnp.ones((16, CHUNK), BF)
    pl.semaphore_wait(barrier, 3)

    def service(g):
        exchange(_done(g - 1), _done(g))

    @pl.loop(0, 8)
    def _(i):
        wait(b.at[pl.ds(0, SHARD)], xs_sem.at[i])
        norm_x(i)

    @pl.loop(0, chunks)
    def _(c):
        @pl.loop(0, 2)
        def _(half):
            s = lax.rem(5 * c + half, 2)

            @pl.when(half == 0)
            def _():
                load_q(1, 1 - s)

            @pl.when(half == 1)
            def _():
                load_kv(1 - s)

            wait(slot.at[s], slot_sem.at[s])
            for n in range(2):
                r = _dot(b[...], slot[s, :, _at(n, 256)])
                for m in range(2):
                    hid[:, pl.ds(_mul(half * 4 + n * 2 + m, HEAD), HEAD)] = turn(r[:, _at(m, HEAD)])

            @pl.when((half == 0) & (c >= 1))
            def _():
                finish(c - 1)

            @pl.when((half == 1) & (c >= 1))
            def _():
                flush()

            service(11 * c + half)

        s = lax.rem(5 * c + 2, 2)
        load_wo(0, 1 - s)
        wait(slot.at[s, :, pl.ds(0, 256)], slot_sem.at[s])
        r = _dot(b[...], slot[s, :, 0:256])
        hid[:, keys] = turn(r[:, :HEAD])
        vt_s[0:HEAD, :] = r[:, HEAD:].astype(BF).T

        @pl.when(c < chunks - 1)
        def _():
            load_x(c + 1)

        attention()
        service(11 * c + 2)

        @pl.loop(0, 2)
        def _(half):
            s = lax.rem(5 * c + 3 + half, 2)

            @pl.when(half == 0)
            def _():
                load_wo(1, 1 - s)

            @pl.when((half == 1) & (c < chunks - 1))
            def _():
                load_q(0, 1 - s)

            @pl.when((half == 1) & (c == chunks - 1))
            def _():
                load_gu(0, 1 - s)

            wait(slot.at[s], slot_sem.at[s])

            @pl.loop(0, 4)
            def _(p):
                i = half * 4 + p
                k = c * PIECES + i

                @pl.when(c < chunks - 1)
                def _():
                    wait(b.at[pl.ds(0, SHARD)], xs_sem.at[i])

                produce(k, lambda n: _dot(seen[...], slot[s, pl.ds(_mul(p * 2 + n, 1024), 1024), :]), lambda: norm_x(i))

                @pl.when(i >= 1)
                def _():
                    add_core(k - 1)

                service(11 * c + 3 + i)

    def fetch_b(c, p):
        fc, fa, fb = 1 - lax.div(p, 4), 1 - lax.rem(p, 2), 1 - lax.rem(lax.div(p, 2), 2)
        fa, fb = fa * fc + fb * (1 - fc), fb * fc + fa * (1 - fc)
        shard = me + fc * d + fa * (a_dev - me) + fb * (b_dev - me)
        start_local(bbuf.at[rows_of(c, shard)], b.at[pl.ds(_mul(p, SHARD), SHARD)], b_sem)

    def arrived(c):
        wait(recva.at[pl.ds(0, 2)], rc.at[c])

    arrived(0)
    for p in range(8):
        fetch_b(0, p)

    @pl.loop(0, chunks)
    def _(c):
        u = h_sums + c
        wait(b, b_sem)

        g = 11 * chunks + 22 * c

        @pl.loop(0, 14)
        def _(t):
            s = lax.rem(t, 2)

            @pl.when(t < 13)
            def _():
                load_gu(t + 1, 1 - s)

            @pl.when(t == 13)
            def _():
                load_d(0, 1 - s)

            wait(slot.at[s], slot_sem.at[s])
            gate = _dot(b[...], slot[s, :, 0:256])
            up = _dot(b[...], slot[s, :, 256:512])
            hid[:, cols_of(t, 256)] = (gate * jax.nn.sigmoid(gate) * up).astype(BF)

            @pl.when(t == 0)
            def _():
                finish(u - 1)

            @pl.when(t == 1)
            def _():
                flush()

            service(g + t)

        @pl.loop(0, 8)
        def _(t):
            s = lax.rem(t, 2)

            @pl.when(t < 7)
            def _():
                load_d(t + 1, 1 - s)

            @pl.when((t == 7) & (c < chunks - 1))
            def _():
                load_gu(0, 1 - s)

            wait(slot.at[s, pl.ds(0, 7168)], slot_sem.at[s])
            k = u * PIECES + t
            produce(k, lambda n: _dot(hid[...], slot[s, pl.ds(n * 3584, 3584), :]))

            @pl.when(t >= 1)
            def _():
                add_core(k - 1)

            @pl.when((t == 7) & (c == chunks - 1))
            def _():
                finish(u)
                flush()

            @pl.when((t == 2) & (c < chunks - 1))
            def _():
                arrived(c + 1)

            @pl.when((t >= 2) & (t < 6) & (c < chunks - 1))
            def _():
                for p in range(2):
                    fetch_b(c + 1, (t - 2) * 2 + p)

            service(g + 14 + t)

    exchange(sum(_counts()), STRIDE * (sums - 1) + WAIT + PIECES + L_Y_A)

    for n in range(4):
        wait(sendb.at[0], b_send.at[n])
    for n in range(2):
        wait(csend.at[0], c_send.at[n])
        for sem in (sh_b, sh_a, sh_c, sh_l):
            wait(shard.at[0], sem.at[n])
    for n in range(3):
        wait(senda.at[0], a_send.at[n])
    for n in range(sums):
        wait(recva.at[pl.ds(0, 2)], fw.at[n])
    for n in range(chunks, sums):
        arrived(n)


def _layer(x, gain_a, wq, wk, wv, wo, gain_m, wg, wu, wd):
    tokens, width = x.shape
    chunks = tokens // CHUNK
    sums, pieces = 2 * chunks, 2 * chunks * PIECES
    angle = np.arange(CHUNK, dtype=np.float32)[:, None] * np.float32(THETA) ** (-np.arange(HEAD // 2, dtype=np.float32) / (HEAD // 2))
    cos, sin = np.cos(angle), np.sin(angle)
    turns = jnp.asarray(np.concatenate([cos, cos, -sin, sin], 1))
    gains = jnp.concatenate([gain_a, gain_m]).astype(F32).reshape(-1, 128)
    any_, vmem = pl.BlockSpec(memory_space=pl.ANY), pl.BlockSpec(memory_space=pltpu.VMEM)
    dma = pltpu.SemaphoreType.DMA
    ff = wg.shape[1]
    matmuls = tokens * (wq.shape[1] * 2 + 2 * HEAD + 3 * ff)
    out = pl.pallas_call(
        _kernel,
        out_shape=[
            jax.ShapeDtypeStruct((tokens, width), BF),
            jax.ShapeDtypeStruct((tokens, width), BF),
            jax.ShapeDtypeStruct((sums, 2 * SHARD, width), BF),
            jax.ShapeDtypeStruct((sums, 2 * SHARD, width), F32),
            jax.ShapeDtypeStruct((sums, SHARD, width), BF),
        ],
        in_specs=[vmem] * 2 + [any_] * 8,
        out_specs=[any_] * 5,
        scratch_shapes=[
            pltpu.VMEM((2, 8192, 512), BF),
            pltpu.VMEM((CHUNK, width), BF),
            pltpu.VMEM((CHUNK, ff), BF),
            pltpu.VMEM((2, width), F32),
            pltpu.VMEM((HEAD + 16, CHUNK), BF),
            pltpu.VMEM((CHUNK, 8 * HEAD), BF),
            pltpu.VMEM((2, 256, COLS), F32),
            pltpu.VMEM((2, 256, COLS), BF),
            pltpu.VMEM((4, 256, COLS), BF),
            pltpu.VMEM((3, 128, width), BF),
            pltpu.VMEM((2, 128, COLS), F32),
            pltpu.VMEM((4, 128, COLS), F32),
            pltpu.VMEM((4, 128, COLS), BF),
            pltpu.VMEM((4, SHARD, COLS), BF),
            pltpu.VMEM((8, SHARD, COLS), F32),
            pltpu.VMEM((4, SHARD, COLS), BF),
            pltpu.VMEM((4, SHARD, COLS), BF),
            pltpu.VMEM((chunks, SHARD, width), BF),
            pltpu.VMEM((2, SHARD, width), BF),
            dma((2,)), dma, dma((8,)),
            dma((2,)), dma((4,)),
            dma((3,)), dma((pieces,)), dma((2,)), dma((4,)), dma((4,)),
            dma((4,)), dma((pieces,)), dma((4,)), dma((4,)),
            dma((2,)), dma((2,)), dma((2,)), dma((2,)),
            dma((pieces,)), dma((pieces // 4,)), dma((sums,)), dma((sums,)),
        ],
        compiler_params=pltpu.CompilerParams(collective_id=0, has_side_effects=True, vmem_limit_bytes=67043328),
        cost_estimate=pl.CostEstimate(flops=2 * width * matmuls, transcendentals=0, bytes_accessed=10**9),
    )(turns, gains, x, wq, wk, wv, wo, wg, wu, wd)
    return out[0]


def solution(mesh):
    def step(x, *rest):
        return _layer(x.reshape(-1, x.shape[-1]), *rest).reshape(x.shape)

    tokens, whole, columns, rows = P("dp", None, None), P(None), P(None, "tp"), P("tp", None)
    return jax.shard_map(
        step,
        mesh=mesh,
        in_specs=(tokens, whole, columns, columns, columns, rows, whole, columns, columns, rows),
        out_specs=tokens,
        check_vma=False,
    )
```

```python
import jax
import jax.numpy as jnp
import numpy as np
from jax import lax
from jax.experimental import pallas as pl
from jax.experimental.pallas import tpu as pltpu
from jax.sharding import PartitionSpec as P

HEAD = 128
THETA = 10000
LOG2E = 1.4426950408889634
HIDDEN = -1e30
EPS = 1e-6

CHUNK = 512
SHARD = 64
COLS = 1024
PIECES = 8
BF, F32 = jnp.bfloat16, jnp.float32

STRIDE, LAG = 16, 4
L_LOAD_A, L_ADD_A = LAG, LAG + 2
L_LOAD_B, L_ADD_B = 2 * LAG + 2, 2 * LAG + 4
L_Y_B, L_Y_A = 3 * LAG + 4, 4 * LAG + 4
L_H, L_H_B, L_H_A = 2 * LAG + 12, 3 * LAG + 12, 4 * LAG + 12
LAST_A, LAST_ADD_A, LAST_B, LAST_ADD_B, LAST_Y_B, LAST_Y_A = 2, 3, 4, 5, 7, 9
PACE = (
    "00001111101212022022111120001000011010100105",
    "2210101011112222101011",
    "0101222221101011011011",
    "1120101111011221112010",
    "1111011222022112210000",
)


def _counts():
    return [int(digit) for digit in "".join(PACE)]


def _words(c, first, steps):
    def packed(n):
        counts, start = _counts(), first + n * steps
        totals = [sum(counts[: start + m]) for m in range(steps + 1)]
        totals += totals[-1:] * 3
        return [totals[m] + sum((totals[m + k] - totals[m]) << (3 + 5 * k) for k in (1, 2, 3)) for m in range(0, steps + 1, 4)]

    words = [packed(n) for n in range(4)]
    return [jnp.where(c < 2, jnp.where(c == 0, w0, w1), jnp.where(c == 2, w2, w3)) for w0, w1, w2, w3 in zip(*words)]


def _total(words, m):
    word = words[-1]
    for n in reversed(range(len(words) - 1)):
        word = jnp.where(m < 4 * n + 4, words[n], word)
    k = m & 3
    return (word & 255) + jnp.where(k == 0, 0, lax.shift_right_logical(word, 3 + 5 * k) & 31)


def _dot(a, b):
    return jnp.dot(a, b, preferred_element_type=F32)


def _at(i, n):
    return slice(i * n, i * n + n)


def _mul(i, n):
    return pl.multiple_of(i * n, n)


def _kernel(turns, gains, x, wq, wk, wv, wo, wg, wu, wd, y, bbuf, recva, reta, recvb,
            slot, b, hid, gain_s, vt_s, seen, own, csend, crecv, senda, retas, rt_l, ra_l, sendb, retb, rb_l, res_l, hsh, shard,
            slot_sem, b_sem, xs_sem, c_send, c_recv, a_send, a_recv, ra_out, la_sem, lt_sem, b_send, b_recv, lb_sem, lr_sem,
            sh_b, sh_a, sh_c, sh_l, from_b, from_a, rc, fw):
    chunks = x.shape[0] // CHUNK
    h_sums, sums = chunks, 2 * chunks
    me = lax.axis_index("tp")
    core, iy, ix = lax.rem(me, 2), lax.rem(lax.div(me, 2), 2), lax.div(me, 4)
    d = 1 - 2 * core
    sib, xn, yn = me + d, me + 4 - 8 * ix, me + 2 - 4 * iy
    a_dev, b_dev = xn * (1 - core) + yn * core, yn * (1 - core) + xn * core
    ab = xn + yn - me

    keys = pl.ds(8 * HEAD, HEAD)

    def remote(src, dst, send, recv, to):
        return pltpu.make_async_remote_copy(src_ref=src, dst_ref=dst, send_sem=send, recv_sem=recv, device_id={"tp": to},
                                            device_id_type=pl.DeviceIdType.MESH)

    def start_local(src, dst, sem):
        pltpu.make_async_copy(src, dst, sem).start()

    def wait(ref, sem):
        pltpu.make_async_copy(ref, ref, sem).wait()

    def cols_of(i, n=COLS):
        return pl.ds(_mul(i, n), n)

    def sixteen(r):
        return pl.ds(_mul(r, 16), 16)

    def thirty_two(r):
        return pl.ds(_mul(r, 32), 32)

    def rows_of(c, shard):
        return pl.ds(_mul(c * 8 + shard, SHARD), SHARD)


    def add_core(k):
        u, i, two = lax.div(k, PIECES), lax.rem(k, PIECES), lax.rem(k, 2)
        a_slot = lax.rem(u, 3)

        @pl.when(i >= 1)
        def _():
            wait(retas.at[0], ra_out.at[1 - two])

        @pl.when((i == 0) & (u >= 3))
        def _():
            wait(senda.at[0], a_send.at[a_slot])

        wait(crecv.at[0], c_recv.at[lax.rem(k, 4)])

        @pl.loop(0, 4)
        def _(r):
            up, lo = thirty_two(r), thirty_two(r + 4)
            senda[a_slot, up, cols_of(i)] = (own[two, up, :] + crecv[lax.rem(k, 4), up, :].astype(F32)).astype(BF)
            retas[two, up, :] = own[two, lo, :] + crecv[lax.rem(k, 4), lo, :].astype(F32)

        start_local(retas.at[two], reta.at[u, :, cols_of(i)], ra_out.at[two])

    def staged(v, fn, first, end):
        i = v & (STRIDE - 1)

        @pl.when((v >= STRIDE * first) & (v < STRIDE * end) & (i < PIECES))
        def _():
            u = lax.div(v, STRIDE)
            fn(u * PIECES + i, u, i)

    def send_a(k, u, i):
        part = senda.at[lax.rem(u, 3), :, cols_of(i)]
        remote(part, recva.at[u, :, cols_of(i)], a_send.at[lax.rem(u, 3)], a_recv.at[k], a_dev).start()

    def load_a(k, u, i):
        four = k & 3
        wait(recva.at[u, :, cols_of(i)], a_recv.at[k])
        start_local(recva.at[u, :, cols_of(i)], ra_l.at[four], la_sem.at[four])
        start_local(reta.at[u, :, cols_of(i)], rt_l.at[four], lt_sem.at[four])

    def add_a(k, u, i):
        four, ring = k & 3, k & 7
        wait(ra_l.at[four], la_sem.at[four])
        wait(rt_l.at[four], lt_sem.at[four])

        @pl.when(k >= 4)
        def _():
            wait(sendb.at[0], b_send.at[four])

        @pl.loop(0, 2)
        def _(r):
            up, lo = thirty_two(r), thirty_two(r + 2)
            sendb[four, up, :] = (rt_l[four, up, :] + ra_l[four, up, :].astype(F32)).astype(BF)
            retb[ring, up, :] = rt_l[four, lo, :] + ra_l[four, lo, :].astype(F32)

        remote(sendb.at[four], recvb.at[u, :, cols_of(i)], b_send.at[four], b_recv.at[k], b_dev).start()

    def load_b(k, u, i):
        four = k & 3
        wait(recvb.at[u, :, cols_of(i)], b_recv.at[k])
        start_local(recvb.at[u, :, cols_of(i)], rb_l.at[four], lb_sem.at[four])

        @pl.when(u < h_sums)
        def _():
            start_local(x.at[rows_of(u, me), cols_of(i)], res_l.at[four], lr_sem.at[four])

    def add_b(k, u, i):
        four, ring, slot_u = k & 3, k & 7, u & 1
        wait(rb_l.at[four], lb_sem.at[four])

        @pl.when((i == 0) & (u >= 2))
        def _():
            for sem in (sh_b, sh_a, sh_c):
                wait(shard.at[0], sem.at[slot_u])

        @pl.when((i == 0) & (u >= h_sums + 2))
        def _():
            wait(shard.at[0], sh_l.at[slot_u])

        @pl.when(u < h_sums)
        def _():
            wait(res_l.at[four], lr_sem.at[four])

            @pl.loop(0, 2)
            def _(r):
                at = thirty_two(r)
                total = retb[ring, at, :] + rb_l[four, at, :].astype(F32)
                hsh[u, at, cols_of(i)] = (res_l[four, at, :].astype(F32) + total).astype(BF)

            @pl.when(i == PIECES - 1)
            def _():
                norm_h(u, slot_u)

        @pl.when(u >= h_sums)
        def _():
            c = u - h_sums

            @pl.loop(0, 2)
            def _(r):
                at = thirty_two(r)
                total = retb[ring, at, :] + rb_l[four, at, :].astype(F32)
                shard[slot_u, at, cols_of(i)] = (hsh[c, at, cols_of(i)].astype(F32) + total).astype(BF)

            send_shard(y, c, k, u, i)

            @pl.when(i == PIECES - 1)
            def _():
                start_local(shard.at[slot_u], y.at[rows_of(c, me)], sh_l.at[slot_u])

    def halves(i):
        return pl.ds(_mul(lax.div(i, 4), 4096), 4096)

    def send_shard(out, c, k, u, i):
        slot_u = lax.rem(u, 2)
        part, mine = shard.at[slot_u, :, cols_of(i)], out.at[rows_of(c, me), cols_of(i)]
        remote(part, mine, sh_b.at[slot_u], from_b.at[k], b_dev).start()
        remote(part, mine, sh_a.at[slot_u], from_a.at[lax.div(k, 4)], a_dev).start()

        @pl.when((i & 3) == 3)
        def _():
            remote(shard.at[slot_u, :, halves(i)], out.at[rows_of(c, me), halves(i)], sh_c.at[slot_u], rc.at[u], sib).start()

    def pass_b(out, c, k, u, i):
        part = out.at[rows_of(c, b_dev), cols_of(i)]
        wait(part, from_b.at[k])
        remote(part, part, fw.at[u], from_a.at[lax.div(k, 4)], a_dev).start()

        @pl.when((i & 3) == 3)
        def _():
            half = out.at[rows_of(c, b_dev), halves(i)]
            remote(half, half, fw.at[u], rc.at[u], sib).start()

    def pass_a(out, c, k, u, i):
        @pl.when((i & 3) == 3)
        def _():
            wait(recva.at[u, :, halves(i)], from_a.at[lax.div(k, 4)])
            for who in (a_dev, ab):
                half = out.at[rows_of(c, who), halves(i)]
                remote(half, half, fw.at[u], rc.at[u], sib).start()

    def norm_rows(src, dst, which, r):
        squares = jnp.zeros((16, 1024), F32)
        for j in range(8):
            wide = src(r, j).astype(F32)
            squares += wide * wide
        scale = lax.rsqrt(jnp.sum(squares, -1, keepdims=True) * (1 / 8192) + EPS)
        for j in range(8):
            dst(r, j, (src(r, j).astype(F32) * scale * gain_s[which : which + 1, _at(j, COLS)]).astype(BF))

    def norm_h(u, slot_u):
        def src(r, j):
            return hsh[u, sixteen(r), _at(j, COLS)]

        def dst(r, j, value):
            shard[slot_u, sixteen(r), _at(j, COLS)] = value

        @pl.loop(0, 4)
        def _(r):
            norm_rows(src, dst, 1, r)

        start_local(shard.at[slot_u], bbuf.at[rows_of(u, me)], sh_l.at[slot_u])

    def send_h(k, u, i):
        send_shard(bbuf, u, k, u, i)

    def pass_h_b(k, u, i):
        @pl.when(i == 0)
        def _():
            wait(shard.at[0], sh_l.at[lax.rem(u, 2)])

        pass_b(bbuf, u, k, u, i)

    def pass_h_a(k, u, i):
        pass_a(bbuf, u, k, u, i)

    def pass_y_b(k, u, i):
        pass_b(y, u - h_sums, k, u, i)

    def pass_y_a(k, u, i):
        pass_a(y, u - h_sums, k, u, i)

    def exchange(first, end):
        @pl.loop(first, end)
        def _(v):
            staged(v, send_a, 0, sums - 1)
            staged(v - L_LOAD_A, load_a, 0, sums - 1)
            staged(v - L_ADD_A, add_a, 0, sums - 1)
            staged(v - L_LOAD_B, load_b, 0, sums - 1)
            staged(v - L_ADD_B, add_b, 0, sums - 1)

            @pl.when((v >= L_H) & (v < STRIDE * (h_sums - 1) + PIECES + L_H_A))
            def _():
                staged(v - L_H, send_h, 0, h_sums)
                staged(v - L_H_B, pass_h_b, 0, h_sums)
                staged(v - L_H_A, pass_h_a, 0, h_sums)

            @pl.when(v >= STRIDE * h_sums + L_Y_B)
            def _():
                staged(v - L_Y_B, pass_y_b, h_sums, sums - 1)
                staged(v - L_Y_A, pass_y_a, h_sums, sums - 1)

    def exchange_last(first, end):
        @pl.loop(first, end)
        def _(v):
            for lag, fn in ((0, send_a), (LAST_A, load_a), (LAST_ADD_A, add_a), (LAST_B, load_b), (LAST_ADD_B, add_b),
                            (LAST_Y_B, pass_y_b), (LAST_Y_A, pass_y_a)):
                i = v - lag

                @pl.when((i >= 0) & (i < PIECES))
                def _(fn=fn, i=i):
                    u = jnp.int32(sums - 1)
                    fn(u * PIECES + i, u, i)


    def load_q(half, s):
        start_local(wq.at[:, cols_of(half, 512)], slot.at[s], slot_sem.at[s])

    def load_kv(s):
        start_local(wk, slot.at[s, :, pl.ds(0, HEAD)], slot_sem.at[s])
        start_local(wv, slot.at[s, :, pl.ds(HEAD, HEAD)], slot_sem.at[s])

    def load_wo(half, s):
        for n in range(8):
            start_local(wo.at[:, cols_of(half * 8 + n, 512)], slot.at[s, pl.ds(n * 1024, 1024)], slot_sem.at[s])

    def load_gu(t, s):
        start_local(wg.at[:, cols_of(t, 256)], slot.at[s, :, pl.ds(0, 256)], slot_sem.at[s])
        start_local(wu.at[:, cols_of(t, 256)], slot.at[s, :, pl.ds(256, 256)], slot_sem.at[s])

    def load_d(t, s):
        for n in range(2):
            start_local(wd.at[:, cols_of(t * 2 + n, 512)], slot.at[s, pl.ds(n * 3584, 3584)], slot_sem.at[s])


    def produce(k, tile, beside=None):
        ring, two = lax.rem(k, 4), lax.rem(k, 2)

        @pl.when(k >= 2)
        def _():
            wait(csend.at[0], c_send.at[two])

        for n in range(2):
            term = tile(n)
            csend[two, :, _at(n, 512)] = term[:256].astype(BF)
            own[two, :, _at(n, 512)] = term[256:]
            if beside and n == 0:
                beside()
        remote(csend.at[two], crecv.at[ring], c_send.at[two], c_recv.at[ring], sib).start()

    def finish(u):
        add_core(u * PIECES + PIECES - 1)

    def flush():
        wait(retas.at[0], ra_out.at[1])

    def turn(t):
        wide = t.astype(BF).astype(F32)
        return (wide * turns[:, :HEAD] + pltpu.roll(wide, HEAD // 2, 1) * turns[:, HEAD:]).astype(BF)

    def load_x(c):
        for i in range(8):
            start_local(x.at[rows_of(c, i)], b.at[pl.ds(i * SHARD, SHARD)], xs_sem.at[i])

    def norm_x(i):
        def src(r, j):
            return b[sixteen(i * 4 + r), _at(j, COLS)]

        def dst(r, j, value):
            b[sixteen(i * 4 + r), _at(j, COLS)] = value

        for r in range(4):
            norm_rows(src, dst, 0, r)

    def attention():
        key = lax.broadcasted_iota(jnp.int32, (256, 256), 0)
        query = lax.broadcasted_iota(jnp.int32, (256, 256), 1)
        ok = key <= query
        e = HEAD**-0.5 * LOG2E

        def place(i):
            iy_, ix_, core_ = (i // 2) % 2, i // 4, i % 2
            fx, fy, fc = (ix_ - ix) * (ix_ - ix), (iy_ - iy) * (iy_ - iy), (core_ - core) * (core_ - core)
            fa, fb = fx * (1 - core) + fy * core, fy * (1 - core) + fx * core
            return (1 - fc) * (7 - 2 * fa - fb) + fc * (3 - fa - 2 * fb)

        def head(h):
            def scores(kb, qb):
                return lax.dot_general(hid[_at(kb, 256), keys], hid[_at(qb, 256), pl.ds(_mul(h, HEAD), HEAD)],
                                       (((1,), (1,)), ((), ())), preferred_element_type=F32)

            def put(qb, total):
                out = (total[:HEAD] * (1 / total[HEAD : HEAD + 1])).T.astype(BF)
                for j in range(4):
                    seen[pl.ds(_mul(place(qb * 4 + j), SHARD), SHARD), pl.ds(_mul(h, HEAD), HEAD)] = out[_at(j, SHARD)]

            s00 = jnp.where(ok, scores(0, 0), HIDDEN)
            s01 = scores(0, 1)
            s11 = jnp.where(ok, scores(1, 1), HIDDEN)
            top0 = jnp.max(s00, axis=0, keepdims=True)
            top1 = jnp.maximum(jnp.max(s01, axis=0, keepdims=True), jnp.max(s11, axis=0, keepdims=True))
            p00 = jnp.exp2((s00 - top0) * e).astype(BF)
            p01 = jnp.exp2((s01 - top1) * e).astype(BF)
            p11 = jnp.exp2((s11 - top1) * e).astype(BF)
            put(0, _dot(vt_s[:, 0:256], p00))
            put(1, _dot(vt_s[:, 0:256], p01) + _dot(vt_s[:, 256:512], p11))

        @pl.loop(0, 4)
        def _(h):
            head(2 * h)
            head(2 * h + 1)


    barrier = pltpu.get_barrier_semaphore()
    for other in (sib, a_dev, b_dev):
        pl.semaphore_signal(barrier, inc=1, device_id={"tp": other}, device_id_type=pl.DeviceIdType.MESH)
    load_x(0)
    load_q(0, 0)
    for n in range(2):
        for j in range(64):
            gain_s[n : n + 1, _at(j, 128)] = gains[n * 64 + j : n * 64 + j + 1, :]
    vt_s[HEAD:, :] = jnp.ones((16, CHUNK), BF)

    def service(words, s):
        exchange(_total(words, s), _total(words, s + 1))

    @pl.loop(0, 8)
    def _(i):
        wait(b.at[pl.ds(0, SHARD)], xs_sem.at[i])
        norm_x(i)

    pl.semaphore_wait(barrier, 3)

    @pl.loop(0, chunks)
    def _(c):
        words = _words(c, 0, 11)
        @pl.loop(0, 2)
        def _(half):
            s = lax.rem(5 * c + half, 2)

            @pl.when(half == 0)
            def _():
                load_q(1, 1 - s)

            @pl.when(half == 1)
            def _():
                load_kv(1 - s)

            wait(slot.at[s], slot_sem.at[s])
            for n in range(2):
                r = _dot(b[...], slot[s, :, _at(n, 256)])
                for m in range(2):
                    hid[:, pl.ds(_mul(half * 4 + n * 2 + m, HEAD), HEAD)] = turn(r[:, _at(m, HEAD)])

            @pl.when((half == 0) & (c >= 1))
            def _():
                finish(c - 1)

            @pl.when((half == 1) & (c >= 1))
            def _():
                flush()

            service(words, half)

        s = lax.rem(5 * c + 2, 2)
        load_wo(0, 1 - s)
        wait(slot.at[s, :, pl.ds(0, 256)], slot_sem.at[s])
        r = _dot(b[...], slot[s, :, 0:256])
        hid[:, keys] = turn(r[:, :HEAD])
        vt_s[0:HEAD, :] = r[:, HEAD:].astype(BF).T

        @pl.when(c < chunks - 1)
        def _():
            load_x(c + 1)

        attention()
        service(words, 2)

        @pl.loop(0, 2)
        def _(half):
            s = lax.rem(5 * c + 3 + half, 2)

            @pl.when(half == 0)
            def _():
                load_wo(1, 1 - s)

            @pl.when((half == 1) & (c < chunks - 1))
            def _():
                load_q(0, 1 - s)

            @pl.when((half == 1) & (c == chunks - 1))
            def _():
                load_gu(0, 1 - s)

            wait(slot.at[s], slot_sem.at[s])

            @pl.loop(0, 4)
            def _(p):
                i = half * 4 + p
                k = c * PIECES + i

                @pl.when(c < chunks - 1)
                def _():
                    wait(b.at[pl.ds(0, SHARD)], xs_sem.at[i])

                produce(k, lambda n: _dot(seen[...], slot[s, pl.ds(_mul(p * 2 + n, 1024), 1024), :]), lambda: norm_x(i))

                @pl.when(i >= 1)
                def _():
                    add_core(k - 1)

                service(words, 3 + i)

    def fetch_b(c, p):
        fc, fa, fb = 1 - lax.div(p, 4), 1 - lax.rem(p, 2), 1 - lax.rem(lax.div(p, 2), 2)
        fa, fb = fa * fc + fb * (1 - fc), fb * fc + fa * (1 - fc)
        shard = me + fc * d + fa * (a_dev - me) + fb * (b_dev - me)
        start_local(bbuf.at[rows_of(c, shard)], b.at[pl.ds(_mul(p, SHARD), SHARD)], b_sem)

    def arrived(c):
        wait(recva.at[pl.ds(0, 2)], rc.at[c])

    for p in range(4):
        fetch_b(0, 4 + p)
    arrived(0)
    for p in range(4):
        fetch_b(0, p)

    @pl.loop(0, chunks)
    def _(c):
        u = h_sums + c
        wait(b, b_sem)

        words = _words(c, 44, 22)

        @pl.loop(0, 14)
        def _(t):
            s = lax.rem(t, 2)

            @pl.when(t < 13)
            def _():
                load_gu(t + 1, 1 - s)

            @pl.when(t == 13)
            def _():
                load_d(0, 1 - s)

            wait(slot.at[s], slot_sem.at[s])
            gate = _dot(b[...], slot[s, :, 0:256])
            up = _dot(b[...], slot[s, :, 256:512])
            hid[:, cols_of(t, 256)] = (gate * jax.nn.sigmoid(gate) * up).astype(BF)

            @pl.when(t == 0)
            def _():
                finish(u - 1)

            @pl.when(t == 1)
            def _():
                flush()

            service(words, t)

        @pl.loop(0, 8)
        def _(t):
            s = lax.rem(t, 2)

            @pl.when(t < 7)
            def _():
                load_d(t + 1, 1 - s)

            @pl.when((t == 7) & (c < chunks - 1))
            def _():
                load_gu(0, 1 - s)

            wait(slot.at[s, pl.ds(0, 7168)], slot_sem.at[s])
            k = u * PIECES + t
            produce(k, lambda n: _dot(hid[...], slot[s, pl.ds(n * 3584, 3584), :]))

            @pl.when(t >= 1)
            def _():
                add_core(k - 1)

            @pl.when((t == 7) & (c == chunks - 1))
            def _():
                finish(u)
                flush()

            @pl.when((t == 2) & (c < chunks - 1))
            def _():
                arrived(c + 1)

            @pl.when((t >= 2) & (t < 6) & (c < chunks - 1))
            def _():
                for p in range(2):
                    fetch_b(c + 1, (t - 2) * 2 + p)

            service(words, 14 + t)

            @pl.when((t >= 1) & (c == chunks - 1))
            def _():
                exchange_last(t - 1, t)

    exchange(sum(_counts()), STRIDE * (sums - 2) + PIECES + L_Y_A)
    exchange_last(PIECES - 1, PIECES + LAST_Y_A)

    for n in range(4):
        wait(sendb.at[0], b_send.at[n])
    for n in range(2):
        wait(csend.at[0], c_send.at[n])
        for sem in (sh_b, sh_a, sh_c, sh_l):
            wait(shard.at[0], sem.at[n])
    for n in range(3):
        wait(senda.at[0], a_send.at[n])
    for n in range(sums):
        wait(recva.at[pl.ds(0, 2)], fw.at[n])
    for n in range(chunks, sums):
        arrived(n)


def _layer(x, gain_a, wq, wk, wv, wo, gain_m, wg, wu, wd):
    tokens, width = x.shape
    chunks = tokens // CHUNK
    sums, pieces = 2 * chunks, 2 * chunks * PIECES
    angle = np.arange(CHUNK, dtype=np.float32)[:, None] * np.float32(THETA) ** (-np.arange(HEAD // 2, dtype=np.float32) / (HEAD // 2))
    cos, sin = np.cos(angle), np.sin(angle)
    turns = jnp.asarray(np.concatenate([cos, cos, -sin, sin], 1))
    gains = jnp.concatenate([gain_a, gain_m]).astype(F32).reshape(-1, 128)
    any_, vmem = pl.BlockSpec(memory_space=pl.ANY), pl.BlockSpec(memory_space=pltpu.VMEM)
    dma = pltpu.SemaphoreType.DMA
    ff = wg.shape[1]
    matmuls = tokens * (wq.shape[1] * 2 + 2 * HEAD + 3 * ff)
    out = pl.pallas_call(
        _kernel,
        out_shape=[
            jax.ShapeDtypeStruct((tokens, width), BF),
            jax.ShapeDtypeStruct((tokens, width), BF),
            jax.ShapeDtypeStruct((sums, 2 * SHARD, width), BF),
            jax.ShapeDtypeStruct((sums, 2 * SHARD, width), F32),
            jax.ShapeDtypeStruct((sums, SHARD, width), BF),
        ],
        in_specs=[vmem] * 2 + [any_] * 8,
        out_specs=[any_] * 5,
        scratch_shapes=[
            pltpu.VMEM((2, 8192, 512), BF),
            pltpu.VMEM((CHUNK, width), BF),
            pltpu.VMEM((CHUNK, ff), BF),
            pltpu.VMEM((2, width), F32),
            pltpu.VMEM((HEAD + 16, CHUNK), BF),
            pltpu.VMEM((CHUNK, 8 * HEAD), BF),
            pltpu.VMEM((2, 256, COLS), F32),
            pltpu.VMEM((2, 256, COLS), BF),
            pltpu.VMEM((4, 256, COLS), BF),
            pltpu.VMEM((3, 128, width), BF),
            pltpu.VMEM((2, 128, COLS), F32),
            pltpu.VMEM((4, 128, COLS), F32),
            pltpu.VMEM((4, 128, COLS), BF),
            pltpu.VMEM((4, SHARD, COLS), BF),
            pltpu.VMEM((8, SHARD, COLS), F32),
            pltpu.VMEM((4, SHARD, COLS), BF),
            pltpu.VMEM((4, SHARD, COLS), BF),
            pltpu.VMEM((chunks, SHARD, width), BF),
            pltpu.VMEM((2, SHARD, width), BF),
            dma((2,)), dma, dma((8,)),
            dma((2,)), dma((4,)),
            dma((3,)), dma((pieces,)), dma((2,)), dma((4,)), dma((4,)),
            dma((4,)), dma((pieces,)), dma((4,)), dma((4,)),
            dma((2,)), dma((2,)), dma((2,)), dma((2,)),
            dma((pieces,)), dma((pieces // 4,)), dma((sums,)), dma((sums,)),
        ],
        compiler_params=pltpu.CompilerParams(collective_id=0, has_side_effects=True, vmem_limit_bytes=67043328),
        cost_estimate=pl.CostEstimate(flops=2 * width * matmuls, transcendentals=0, bytes_accessed=10**9),
    )(turns, gains, x, wq, wk, wv, wo, wg, wu, wd)
    return out[0]


def solution(mesh):
    def step(x, *rest):
        return _layer(x.reshape(-1, x.shape[-1]), *rest).reshape(x.shape)

    tokens, whole, columns, rows = P("dp", None, None), P(None), P(None, "tp"), P("tp", None)
    return jax.shard_map(
        step,
        mesh=mesh,
        in_specs=(tokens, whole, columns, columns, columns, rows, whole, columns, columns, rows),
        out_specs=tokens,
        check_vma=False,
    )
```

```python
import jax
import jax.numpy as jnp
import numpy as np
from jax import lax
from jax.experimental import pallas as pl
from jax.experimental.pallas import tpu as pltpu
from jax.sharding import PartitionSpec as P

HEAD = 128
THETA = 10000
LOG2E = 1.4426950408889634
HIDDEN = -1e30
EPS = 1e-6

CHUNK = 512
SHARD = 64
COLS = 1024
PIECES = 8
BF, F32 = jnp.bfloat16, jnp.float32

STRIDE, LAG = 16, 4
L_LOAD_A, L_ADD_A = LAG, LAG + 2
L_LOAD_B, L_ADD_B = 2 * LAG + 2, 2 * LAG + 4
L_Y_B, L_Y_A = 3 * LAG + 4, 4 * LAG + 4
L_H, L_H_B, L_H_A = 2 * LAG + 12, 3 * LAG + 12, 4 * LAG + 12
LAST_A, LAST_ADD_A, LAST_B, LAST_ADD_B, LAST_Y_B, LAST_Y_A = 2, 3, 4, 5, 7, 9
PACE = (
    "00001111101212022022111120001000011010100105",
    "2210101011112222101011",
    "0101222221101011011011",
    "1120101111011221112010",
    "1111011222022112210000",
)


def _counts():
    return [int(digit) for digit in "".join(PACE)]


def _words(c, first, steps):
    def packed(n):
        counts, start = _counts(), first + n * steps
        totals = [sum(counts[: start + m]) for m in range(steps + 1)]
        totals += totals[-1:] * 3
        return [totals[m] + sum((totals[m + k] - totals[m]) << (3 + 5 * k) for k in (1, 2, 3)) for m in range(0, steps + 1, 4)]

    words = [packed(n) for n in range(4)]
    return [jnp.where(c < 2, jnp.where(c == 0, w0, w1), jnp.where(c == 2, w2, w3)) for w0, w1, w2, w3 in zip(*words)]


def _total(words, m):
    word = words[-1]
    for n in reversed(range(len(words) - 1)):
        word = jnp.where(m < 4 * n + 4, words[n], word)
    k = m & 3
    return (word & 255) + jnp.where(k == 0, 0, lax.shift_right_logical(word, 3 + 5 * k) & 31)


def _dot(a, b):
    return jnp.dot(a, b, preferred_element_type=F32)


def _at(i, n):
    return slice(i * n, i * n + n)


def _mul(i, n):
    return pl.multiple_of(i * n, n)


def _kernel(turns, gain_a, gain_m, x, wq, wk, wv, wo, wg, wu, wd, y, bbuf, recva, reta, recvb,
            slot, b, hid, gain_s, vt_s, seen, own, csend, crecv, senda, retas, rt_l, ra_l, sendb, retb, rb_l, res_l, hsh, shard,
            slot_sem, b_sem, xs_sem, c_send, c_recv, a_send, a_recv, ra_out, la_sem, lt_sem, b_send, b_recv, lb_sem, lr_sem,
            sh_b, sh_a, sh_c, sh_l, from_b, from_a, rc, fw):
    chunks = x.shape[0] // CHUNK
    h_sums, sums = chunks, 2 * chunks
    me = lax.axis_index("tp")
    core, iy, ix = lax.rem(me, 2), lax.rem(lax.div(me, 2), 2), lax.div(me, 4)
    d = 1 - 2 * core
    sib, xn, yn = me + d, me + 4 - 8 * ix, me + 2 - 4 * iy
    a_dev, b_dev = xn * (1 - core) + yn * core, yn * (1 - core) + xn * core
    ab = xn + yn - me

    keys = pl.ds(8 * HEAD, HEAD)

    def remote(src, dst, send, recv, to):
        return pltpu.make_async_remote_copy(src_ref=src, dst_ref=dst, send_sem=send, recv_sem=recv, device_id={"tp": to},
                                            device_id_type=pl.DeviceIdType.MESH)

    def start_local(src, dst, sem):
        pltpu.make_async_copy(src, dst, sem).start()

    def wait(ref, sem):
        pltpu.make_async_copy(ref, ref, sem).wait()

    def cols_of(i, n=COLS):
        return pl.ds(_mul(i, n), n)

    def sixteen(r):
        return pl.ds(_mul(r, 16), 16)

    def thirty_two(r):
        return pl.ds(_mul(r, 32), 32)

    def rows_of(c, shard):
        return pl.ds(_mul(c * 8 + shard, SHARD), SHARD)


    def add_core(k):
        u, i, two = lax.div(k, PIECES), lax.rem(k, PIECES), lax.rem(k, 2)
        a_slot = lax.rem(u, 3)

        @pl.when(i >= 1)
        def _():
            wait(retas.at[0], ra_out.at[1 - two])

        @pl.when((i == 0) & (u >= 3))
        def _():
            wait(senda.at[0], a_send.at[a_slot])

        wait(crecv.at[0], c_recv.at[lax.rem(k, 4)])

        @pl.loop(0, 4)
        def _(r):
            up, lo = thirty_two(r), thirty_two(r + 4)
            senda[a_slot, up, cols_of(i)] = (own[two, up, :] + crecv[lax.rem(k, 4), up, :].astype(F32)).astype(BF)
            retas[two, up, :] = own[two, lo, :] + crecv[lax.rem(k, 4), lo, :].astype(F32)

        start_local(retas.at[two], reta.at[u, :, cols_of(i)], ra_out.at[two])

    def staged(v, fn, first, end):
        i = v & (STRIDE - 1)

        @pl.when((v >= STRIDE * first) & (v < STRIDE * end) & (i < PIECES))
        def _():
            u = lax.div(v, STRIDE)
            fn(u * PIECES + i, u, i)

    def send_a(k, u, i):
        part = senda.at[lax.rem(u, 3), :, cols_of(i)]
        remote(part, recva.at[u, :, cols_of(i)], a_send.at[lax.rem(u, 3)], a_recv.at[k], a_dev).start()

    def load_a(k, u, i):
        four = k & 3
        wait(recva.at[u, :, cols_of(i)], a_recv.at[k])
        start_local(recva.at[u, :, cols_of(i)], ra_l.at[four], la_sem.at[four])
        start_local(reta.at[u, :, cols_of(i)], rt_l.at[four], lt_sem.at[four])

    def add_a(k, u, i):
        four, ring = k & 3, k & 7
        wait(ra_l.at[four], la_sem.at[four])
        wait(rt_l.at[four], lt_sem.at[four])

        @pl.when(k >= 4)
        def _():
            wait(sendb.at[0], b_send.at[four])

        @pl.loop(0, 2)
        def _(r):
            up, lo = thirty_two(r), thirty_two(r + 2)
            sendb[four, up, :] = (rt_l[four, up, :] + ra_l[four, up, :].astype(F32)).astype(BF)
            retb[ring, up, :] = rt_l[four, lo, :] + ra_l[four, lo, :].astype(F32)

        remote(sendb.at[four], recvb.at[u, :, cols_of(i)], b_send.at[four], b_recv.at[k], b_dev).start()

    def load_b(k, u, i):
        four = k & 3
        wait(recvb.at[u, :, cols_of(i)], b_recv.at[k])
        start_local(recvb.at[u, :, cols_of(i)], rb_l.at[four], lb_sem.at[four])

        @pl.when(u < h_sums)
        def _():
            start_local(x.at[rows_of(u, me), cols_of(i)], res_l.at[four], lr_sem.at[four])

    def add_b(k, u, i):
        four, ring, slot_u = k & 3, k & 7, u & 1
        wait(rb_l.at[four], lb_sem.at[four])

        @pl.when((i == 0) & (u >= 2))
        def _():
            for sem in (sh_b, sh_a, sh_c):
                wait(shard.at[0], sem.at[slot_u])

        @pl.when((i == 0) & (u >= h_sums + 2))
        def _():
            wait(shard.at[0], sh_l.at[slot_u])

        @pl.when(u < h_sums)
        def _():
            wait(res_l.at[four], lr_sem.at[four])

            @pl.loop(0, 2)
            def _(r):
                at = thirty_two(r)
                total = retb[ring, at, :] + rb_l[four, at, :].astype(F32)
                hsh[u, at, cols_of(i)] = (res_l[four, at, :].astype(F32) + total).astype(BF)

            @pl.when(i == PIECES - 1)
            def _():
                norm_h(u, slot_u)

        @pl.when(u >= h_sums)
        def _():
            c = u - h_sums

            @pl.loop(0, 2)
            def _(r):
                at = thirty_two(r)
                total = retb[ring, at, :] + rb_l[four, at, :].astype(F32)
                shard[slot_u, at, cols_of(i)] = (hsh[c, at, cols_of(i)].astype(F32) + total).astype(BF)

            send_shard(y, c, k, u, i)

            @pl.when(i == PIECES - 1)
            def _():
                start_local(shard.at[slot_u], y.at[rows_of(c, me)], sh_l.at[slot_u])

    def halves(i):
        return pl.ds(_mul(lax.div(i, 4), 4096), 4096)

    def send_shard(out, c, k, u, i):
        slot_u = lax.rem(u, 2)
        part, mine = shard.at[slot_u, :, cols_of(i)], out.at[rows_of(c, me), cols_of(i)]
        remote(part, mine, sh_b.at[slot_u], from_b.at[k], b_dev).start()
        remote(part, mine, sh_a.at[slot_u], from_a.at[lax.div(k, 4)], a_dev).start()

        @pl.when((i & 3) == 3)
        def _():
            remote(shard.at[slot_u, :, halves(i)], out.at[rows_of(c, me), halves(i)], sh_c.at[slot_u], rc.at[u], sib).start()

    def pass_b(out, c, k, u, i):
        part = out.at[rows_of(c, b_dev), cols_of(i)]
        wait(part, from_b.at[k])
        remote(part, part, fw.at[u], from_a.at[lax.div(k, 4)], a_dev).start()

        @pl.when((i & 3) == 3)
        def _():
            half = out.at[rows_of(c, b_dev), halves(i)]
            remote(half, half, fw.at[u], rc.at[u], sib).start()

    def pass_a(out, c, k, u, i):
        @pl.when((i & 3) == 3)
        def _():
            wait(recva.at[u, :, halves(i)], from_a.at[lax.div(k, 4)])
            for who in (a_dev, ab):
                half = out.at[rows_of(c, who), halves(i)]
                remote(half, half, fw.at[u], rc.at[u], sib).start()

    def norm_rows(src, dst, which, r):
        squares = jnp.zeros((16, 1024), F32)
        for j in range(8):
            wide = src(r, j).astype(F32)
            squares += wide * wide
        scale = lax.rsqrt(jnp.sum(squares, -1, keepdims=True) * (1 / 8192) + EPS)
        for j in range(8):
            dst(r, j, (src(r, j).astype(F32) * scale * gain_s[which : which + 1, _at(j, COLS)]).astype(BF))

    def norm_h(u, slot_u):
        def src(r, j):
            return hsh[u, sixteen(r), _at(j, COLS)]

        def dst(r, j, value):
            shard[slot_u, sixteen(r), _at(j, COLS)] = value

        @pl.loop(0, 4)
        def _(r):
            norm_rows(src, dst, 1, r)

        start_local(shard.at[slot_u], bbuf.at[rows_of(u, me)], sh_l.at[slot_u])

    def send_h(k, u, i):
        send_shard(bbuf, u, k, u, i)

    def pass_h_b(k, u, i):
        @pl.when(i == 0)
        def _():
            wait(shard.at[0], sh_l.at[lax.rem(u, 2)])

        pass_b(bbuf, u, k, u, i)

    def pass_h_a(k, u, i):
        pass_a(bbuf, u, k, u, i)

    def pass_y_b(k, u, i):
        pass_b(y, u - h_sums, k, u, i)

    def pass_y_a(k, u, i):
        pass_a(y, u - h_sums, k, u, i)

    def exchange(first, end):
        @pl.loop(first, end)
        def _(v):
            staged(v, send_a, 0, sums - 1)
            staged(v - L_LOAD_A, load_a, 0, sums - 1)
            staged(v - L_ADD_A, add_a, 0, sums - 1)
            staged(v - L_LOAD_B, load_b, 0, sums - 1)
            staged(v - L_ADD_B, add_b, 0, sums - 1)

            @pl.when((v >= L_H) & (v < STRIDE * (h_sums - 1) + PIECES + L_H_A))
            def _():
                staged(v - L_H, send_h, 0, h_sums)
                staged(v - L_H_B, pass_h_b, 0, h_sums)
                staged(v - L_H_A, pass_h_a, 0, h_sums)

            @pl.when(v >= STRIDE * h_sums + L_Y_B)
            def _():
                staged(v - L_Y_B, pass_y_b, h_sums, sums - 1)
                staged(v - L_Y_A, pass_y_a, h_sums, sums - 1)

    def exchange_last(first, end):
        @pl.loop(first, end)
        def _(v):
            for lag, fn in ((0, send_a), (LAST_A, load_a), (LAST_ADD_A, add_a), (LAST_B, load_b), (LAST_ADD_B, add_b),
                            (LAST_Y_B, pass_y_b), (LAST_Y_A, pass_y_a)):
                i = v - lag

                @pl.when((i >= 0) & (i < PIECES))
                def _(fn=fn, i=i):
                    u = jnp.int32(sums - 1)
                    fn(u * PIECES + i, u, i)


    def load_q(half, s):
        start_local(wq.at[:, cols_of(half, 512)], slot.at[s], slot_sem.at[s])

    def load_kv(s):
        start_local(wk, slot.at[s, :, pl.ds(0, HEAD)], slot_sem.at[s])
        start_local(wv, slot.at[s, :, pl.ds(HEAD, HEAD)], slot_sem.at[s])

    def load_wo(half, s):
        for n in range(8):
            start_local(wo.at[:, cols_of(half * 8 + n, 512)], slot.at[s, cols_of(n)], slot_sem.at[s])

    def load_gu(t, s):
        start_local(wg.at[:, cols_of(t, 256)], slot.at[s, :, pl.ds(0, 256)], slot_sem.at[s])
        start_local(wu.at[:, cols_of(t, 256)], slot.at[s, :, pl.ds(256, 256)], slot_sem.at[s])

    def load_d(t, s):
        for n in range(2):
            start_local(wd.at[:, cols_of(t * 2 + n, 512)], slot.at[s, pl.ds(n * 3584, 3584)], slot_sem.at[s])


    def produce(k, tile, beside=None):
        ring, two = lax.rem(k, 4), lax.rem(k, 2)

        @pl.when(k >= 2)
        def _():
            wait(csend.at[0], c_send.at[two])

        for n in range(2):
            term = tile(n)
            csend[two, :, _at(n, 512)] = term[:256].astype(BF)
            own[two, :, _at(n, 512)] = term[256:]
            if beside and n == 0:
                beside()
        remote(csend.at[two], crecv.at[ring], c_send.at[two], c_recv.at[ring], sib).start()

    def finish(u):
        add_core(u * PIECES + PIECES - 1)

    def flush():
        wait(retas.at[0], ra_out.at[1])

    def turn(t):
        wide = t.astype(BF).astype(F32)
        return (wide * turns[:, :HEAD] + pltpu.roll(wide, HEAD // 2, 1) * turns[:, HEAD:]).astype(BF)

    def load_x(c):
        for i in range(8):
            start_local(x.at[rows_of(c, i)], b.at[pl.ds(i * SHARD, SHARD)], xs_sem.at[i])

    def norm_x(i):
        def src(r, j):
            return b[sixteen(i * 4 + r), _at(j, COLS)]

        def dst(r, j, value):
            b[sixteen(i * 4 + r), _at(j, COLS)] = value

        for r in range(4):
            norm_rows(src, dst, 0, r)

    def attention():
        key = lax.broadcasted_iota(jnp.int32, (256, 256), 0)
        query = lax.broadcasted_iota(jnp.int32, (256, 256), 1)
        ok = key <= query
        e = HEAD**-0.5 * LOG2E

        def place(i):
            iy_, ix_, core_ = (i // 2) % 2, i // 4, i % 2
            fx, fy, fc = (ix_ - ix) * (ix_ - ix), (iy_ - iy) * (iy_ - iy), (core_ - core) * (core_ - core)
            fa, fb = fx * (1 - core) + fy * core, fy * (1 - core) + fx * core
            return (1 - fc) * (7 - 2 * fa - fb) + fc * (3 - fa - 2 * fb)

        def head(h):
            def scores(kb, qb):
                return lax.dot_general(hid[_at(kb, 256), keys], hid[_at(qb, 256), cols_of(h, HEAD)],
                                       (((1,), (1,)), ((), ())), preferred_element_type=F32)

            def put(qb, total):
                out = (total[:HEAD] * (1 / total[HEAD : HEAD + 1])).T.astype(BF)
                for j in range(4):
                    seen[pl.ds(_mul(place(qb * 4 + j), SHARD), SHARD), cols_of(h, HEAD)] = out[_at(j, SHARD)]

            s00 = jnp.where(ok, scores(0, 0), HIDDEN)
            s01 = scores(0, 1)
            s11 = jnp.where(ok, scores(1, 1), HIDDEN)
            top0 = jnp.max(s00, axis=0, keepdims=True)
            top1 = jnp.maximum(jnp.max(s01, axis=0, keepdims=True), jnp.max(s11, axis=0, keepdims=True))
            p00 = jnp.exp2((s00 - top0) * e).astype(BF)
            p01 = jnp.exp2((s01 - top1) * e).astype(BF)
            p11 = jnp.exp2((s11 - top1) * e).astype(BF)
            put(0, _dot(vt_s[:, 0:256], p00))
            put(1, _dot(vt_s[:, 0:256], p01) + _dot(vt_s[:, 256:512], p11))

        @pl.loop(0, 4)
        def _(h):
            head(2 * h)
            head(2 * h + 1)


    barrier = pltpu.get_barrier_semaphore()
    for other in (sib, a_dev, b_dev):
        pl.semaphore_signal(barrier, inc=1, device_id={"tp": other}, device_id_type=pl.DeviceIdType.MESH)
    load_x(0)
    load_q(0, 0)
    for n, gain in enumerate((gain_a, gain_m)):
        wide = gain[...].astype(F32)
        for j in range(64):
            gain_s[n : n + 1, _at(j, 128)] = wide[j : j + 1, :]
    vt_s[HEAD:, :] = jnp.ones((16, CHUNK), BF)

    def service(words, s):
        exchange(_total(words, s), _total(words, s + 1))

    @pl.loop(0, 8)
    def _(i):
        wait(b.at[pl.ds(0, SHARD)], xs_sem.at[i])
        norm_x(i)

    pl.semaphore_wait(barrier, 3)

    @pl.loop(0, chunks)
    def _(c):
        words = _words(c, 0, 11)
        @pl.loop(0, 2)
        def _(half):
            s = lax.rem(5 * c + half, 2)

            @pl.when(half == 0)
            def _():
                load_q(1, 1 - s)

            @pl.when(half == 1)
            def _():
                load_kv(1 - s)

            wait(slot.at[s], slot_sem.at[s])
            for n in range(2):
                r = _dot(b[...], slot[s, :, _at(n, 256)])
                for m in range(2):
                    hid[:, cols_of(half * 4 + n * 2 + m, HEAD)] = turn(r[:, _at(m, HEAD)])

            @pl.when((half == 0) & (c >= 1))
            def _():
                finish(c - 1)

            @pl.when((half == 1) & (c >= 1))
            def _():
                flush()

            service(words, half)

        s = lax.rem(5 * c + 2, 2)
        load_wo(0, 1 - s)
        wait(slot.at[s, :, pl.ds(0, 256)], slot_sem.at[s])
        r = _dot(b[...], slot[s, :, 0:256])
        hid[:, keys] = turn(r[:, :HEAD])
        vt_s[0:HEAD, :] = r[:, HEAD:].astype(BF).T

        @pl.when(c < chunks - 1)
        def _():
            load_x(c + 1)

        attention()
        service(words, 2)

        @pl.loop(0, 2)
        def _(half):
            s = lax.rem(5 * c + 3 + half, 2)

            @pl.when(half == 0)
            def _():
                load_wo(1, 1 - s)

            @pl.when((half == 1) & (c < chunks - 1))
            def _():
                load_q(0, 1 - s)

            @pl.when((half == 1) & (c == chunks - 1))
            def _():
                load_gu(0, 1 - s)

            wait(slot.at[s], slot_sem.at[s])

            @pl.loop(0, 4)
            def _(p):
                i = half * 4 + p
                k = c * PIECES + i

                @pl.when(c < chunks - 1)
                def _():
                    wait(b.at[pl.ds(0, SHARD)], xs_sem.at[i])

                produce(k, lambda n: _dot(seen[...], slot[s, pl.ds(_mul(p * 2 + n, 1024), 1024), :]), lambda: norm_x(i))

                @pl.when(i >= 1)
                def _():
                    add_core(k - 1)

                service(words, 3 + i)

    def fetch_b(c, p):
        low, mid, high = p & 1, lax.div(p & 2, 2), lax.div(p, 4)
        to_a, to_b = jnp.where(high == 1, mid, low), jnp.where(high == 1, low, mid)
        shard = ab + d + high * (me - sib) + to_a * (me - a_dev) + to_b * (me - b_dev)
        start_local(bbuf.at[rows_of(c, shard)], b.at[pl.ds(_mul(p, SHARD), SHARD)], b_sem)

    whole = recva.at[pl.ds(0, 2)]

    def arrived(c):
        wait(whole, rc.at[c])

    for p in range(4):
        fetch_b(0, 4 + p)
    arrived(0)
    for p in range(4):
        fetch_b(0, p)

    @pl.loop(0, chunks)
    def _(c):
        u = h_sums + c
        wait(b, b_sem)

        words = _words(c, 44, 22)

        @pl.loop(0, 14)
        def _(t):
            s = lax.rem(t, 2)

            @pl.when(t < 13)
            def _():
                load_gu(t + 1, 1 - s)

            @pl.when(t == 13)
            def _():
                load_d(0, 1 - s)

            wait(slot.at[s], slot_sem.at[s])
            gate = _dot(b[...], slot[s, :, 0:256])
            up = _dot(b[...], slot[s, :, 256:512])
            hid[:, cols_of(t, 256)] = (gate * jax.nn.sigmoid(gate) * up).astype(BF)

            @pl.when(t == 0)
            def _():
                finish(u - 1)

            @pl.when(t == 1)
            def _():
                flush()

            service(words, t)

        @pl.loop(0, 8)
        def _(t):
            s = lax.rem(t, 2)

            @pl.when(t < 7)
            def _():
                load_d(t + 1, 1 - s)

            @pl.when((t == 7) & (c < chunks - 1))
            def _():
                load_gu(0, 1 - s)

            wait(slot.at[s, pl.ds(0, 7168)], slot_sem.at[s])
            k = u * PIECES + t
            produce(k, lambda n: _dot(hid[...], slot[s, pl.ds(n * 3584, 3584), :]))

            @pl.when(t >= 1)
            def _():
                add_core(k - 1)

            @pl.when((t == 7) & (c == chunks - 1))
            def _():
                finish(u)
                flush()

            @pl.when((t == 2) & (c < chunks - 1))
            def _():
                arrived(c + 1)

            @pl.when((t >= 2) & (t < 6) & (c < chunks - 1))
            def _():
                for p in range(2):
                    fetch_b(c + 1, (t - 2) * 2 + p)

            service(words, 14 + t)

            @pl.when((t >= 1) & (c == chunks - 1))
            def _():
                exchange_last(t - 1, t)

    exchange(sum(_counts()), STRIDE * (sums - 2) + PIECES + L_Y_A)
    exchange_last(PIECES - 1, PIECES + LAST_Y_A)

    for n in range(4):
        wait(sendb.at[0], b_send.at[n])
    for n in range(2):
        wait(csend.at[0], c_send.at[n])
        for sem in (sh_b, sh_a, sh_c, sh_l):
            wait(shard.at[0], sem.at[n])
    for n in range(3):
        wait(senda.at[0], a_send.at[n])
    for n in range(sums):
        wait(whole, fw.at[n])
    for n in range(chunks, sums):
        arrived(n)


def _layer(x, gain_a, wq, wk, wv, wo, gain_m, wg, wu, wd):
    tokens, width = x.shape
    chunks = tokens // CHUNK
    sums, pieces = 2 * chunks, 2 * chunks * PIECES
    angle = np.arange(CHUNK, dtype=np.float32)[:, None] * np.float32(THETA) ** (-np.arange(HEAD // 2, dtype=np.float32) / (HEAD // 2))
    cos, sin = np.cos(angle), np.sin(angle)
    turns = jnp.asarray(np.concatenate([cos, cos, -sin, sin], 1))
    gains = [gain.reshape(-1, 128) for gain in (gain_a, gain_m)]
    any_, vmem = pl.BlockSpec(memory_space=pl.ANY), pl.BlockSpec(memory_space=pltpu.VMEM)
    dma = pltpu.SemaphoreType.DMA
    ff = wg.shape[1]
    matmuls = tokens * (wq.shape[1] + wo.shape[0] + wk.shape[1] + wv.shape[1] + ff + ff + ff)
    out = pl.pallas_call(
        _kernel,
        out_shape=[
            jax.ShapeDtypeStruct((tokens, width), BF),
            jax.ShapeDtypeStruct((tokens, width), BF),
            jax.ShapeDtypeStruct((sums, 2 * SHARD, width), BF),
            jax.ShapeDtypeStruct((sums, 2 * SHARD, width), F32),
            jax.ShapeDtypeStruct((sums, SHARD, width), BF),
        ],
        in_specs=[vmem] * 3 + [any_] * 8,
        out_specs=[any_] * 5,
        scratch_shapes=[
            pltpu.VMEM((2, 8192, 512), BF),
            pltpu.VMEM((CHUNK, width), BF),
            pltpu.VMEM((CHUNK, ff), BF),
            pltpu.VMEM((2, width), F32),
            pltpu.VMEM((HEAD + 16, CHUNK), BF),
            pltpu.VMEM((CHUNK, 8 * HEAD), BF),
            pltpu.VMEM((2, 256, COLS), F32),
            pltpu.VMEM((2, 256, COLS), BF),
            pltpu.VMEM((4, 256, COLS), BF),
            pltpu.VMEM((3, 128, width), BF),
            pltpu.VMEM((2, 128, COLS), F32),
            pltpu.VMEM((4, 128, COLS), F32),
            pltpu.VMEM((4, 128, COLS), BF),
            pltpu.VMEM((4, SHARD, COLS), BF),
            pltpu.VMEM((8, SHARD, COLS), F32),
            pltpu.VMEM((4, SHARD, COLS), BF),
            pltpu.VMEM((4, SHARD, COLS), BF),
            pltpu.VMEM((chunks, SHARD, width), BF),
            pltpu.VMEM((2, SHARD, width), BF),
            dma((2,)), dma, dma((8,)),
            dma((2,)), dma((4,)),
            dma((3,)), dma((pieces,)), dma((2,)), dma((4,)), dma((4,)),
            dma((4,)), dma((pieces,)), dma((4,)), dma((4,)),
            dma((2,)), dma((2,)), dma((2,)), dma((2,)),
            dma((pieces,)), dma((pieces // 4,)), dma((sums,)), dma((sums,)),
        ],
        compiler_params=pltpu.CompilerParams(collective_id=0, has_side_effects=True, vmem_limit_bytes=67043328),
        cost_estimate=pl.CostEstimate(flops=2 * width * matmuls, transcendentals=0, bytes_accessed=width * matmuls // tokens),
    )(turns, *gains, x, wq, wk, wv, wo, wg, wu, wd)
    return out[0]


def solution(mesh):
    def step(x, *rest):
        return _layer(x.reshape(-1, x.shape[-1]), *rest).reshape(x.shape)

    tokens, whole, columns, rows = P("dp", None, None), P(None), P(None, "tp"), P("tp", None)
    return jax.shard_map(
        step,
        mesh=mesh,
        in_specs=(tokens, whole, columns, columns, columns, rows, whole, columns, columns, rows),
        out_specs=tokens,
        check_vma=False,
    )
```
